8 devices in a mesh: dp: 1 (over z), tp: 8 (over y, x, core).
Axes of the slice: x: 2, y: 2, z: 1, core: 2. Of those that a mesh axis runs over, the one named last changes fastest.
Arguments:
- x: bfloat16 [256, 2048], P('dp')
- ln_attn_gamma: float32 [2048], replicated
- ln_attn_beta: float32 [2048], replicated
- ln_mlp_gamma: float32 [2048], replicated
- ln_mlp_beta: float32 [2048], replicated
- w_qkv: bfloat16 [2048, 16, 3, 128], P(None, 'tp')
- w_out: bfloat16 [16, 1, 128, 2048], P('tp')
- w_up: bfloat16 [2048, 8192], P(None, 'tp')
- w_down: bfloat16 [8192, 2048], P('tp')
- k_cache: bfloat16 [256, 16, 128, 128], P('dp', 'tp')
- v_cache: bfloat16 [256, 16, 128, 128], P('dp', 'tp')
- positions: int32 [256], P('dp')
Outputs:
- output 1: bfloat16 [256, 2048], P('dp')
- output 2: bfloat16 [256, 16, 128, 128], P('dp', 'tp')
- output 3: bfloat16 [256, 16, 128, 128], P('dp', 'tp')
All inputs are finite; a program needn't handle non-finite values.
Results may differ from the reference program's by a relative error of at most 0.0110546.
Values are sent between devices in bfloat16 or wider.
A program may use at most 1 GiB of HBM per device.

```python
import math
import jax
import jax.numpy as jnp
from jax import lax

D = 2048
GROUPS = 16
QPG = 1
HEAD = 128
FF = 8192
BATCH = 256
SEQ = 128

QKV_SLOTS = QPG + 2
HALF_HEAD = HEAD // 2
SCORE_SCALE = 1.0 / math.sqrt(HEAD)
LN_EPS = 1e-5
ROPE_BASE = 10000.0
NEG_BIG = -1e30


def setup_inputs(seed: int = 0, part: int = 0) -> dict:
    shared_key, part_base = jax.random.split(jax.random.key(seed))
    shared = jax.random.split(shared_key, 8)
    local = jax.random.split(jax.random.fold_in(part_base, part), 8)
    x = jax.random.normal(local[0], (BATCH, D), jnp.float32).astype(jnp.bfloat16)
    ln_attn_gamma = 1.0 + 0.3 * jax.random.normal(shared[0], (D,), jnp.float32)
    ln_attn_beta = 0.3 * jax.random.normal(shared[1], (D,), jnp.float32)
    ln_mlp_gamma = 1.0 + 0.3 * jax.random.normal(shared[2], (D,), jnp.float32)
    ln_mlp_beta = 0.3 * jax.random.normal(shared[3], (D,), jnp.float32)
    w_qkv = (jax.random.normal(shared[4], (D, GROUPS, QKV_SLOTS, HEAD), jnp.float32) * D ** -0.5).astype(jnp.bfloat16)
    w_out = (jax.random.normal(shared[5], (GROUPS, QPG, HEAD, D), jnp.float32) * (GROUPS * QPG * HEAD) ** -0.5).astype(jnp.bfloat16)
    w_up = (jax.random.normal(shared[6], (D, FF), jnp.float32) * D ** -0.5).astype(jnp.bfloat16)
    w_down = (jax.random.normal(shared[7], (FF, D), jnp.float32) * FF ** -0.5).astype(jnp.bfloat16)
    ramp = (2.0 * jnp.arange(SEQ, dtype=jnp.float32) / SEQ - 1.0)[None, None, :, None]
    k_slope = 1.5 * jax.random.normal(local[1], (BATCH, GROUPS, 1, HEAD), jnp.float32)
    k_cache = (jax.random.normal(local[2], (BATCH, GROUPS, SEQ, HEAD), jnp.float32) + ramp * k_slope).astype(jnp.bfloat16)
    v_level = jax.random.normal(local[3], (BATCH, GROUPS, 1, HEAD), jnp.float32)
    v_slope = jax.random.normal(local[4], (BATCH, GROUPS, 1, HEAD), jnp.float32)
    v_cache = (0.5 * jax.random.normal(local[5], (BATCH, GROUPS, SEQ, HEAD), jnp.float32) + v_level + ramp * v_slope).astype(jnp.bfloat16)
    positions = jax.random.randint(local[6], (BATCH,), SEQ // 4, SEQ, dtype=jnp.int32)
    positions = positions.at[0].set(SEQ - 1).at[1].set(SEQ // 4)
    return {'x': x, 'ln_attn_gamma': ln_attn_gamma, 'ln_attn_beta': ln_attn_beta, 'ln_mlp_gamma': ln_mlp_gamma, 'ln_mlp_beta': ln_mlp_beta, 'w_qkv': w_qkv, 'w_out': w_out, 'w_up': w_up, 'w_down': w_down, 'k_cache': k_cache, 'v_cache': v_cache, 'positions': positions}


def layer_norm(act_rows, ln_gamma, ln_beta):
    rows_f32 = act_rows.astype(jnp.float32)
    row_mean = jnp.mean(rows_f32, axis=-1, keepdims=True)
    centred = rows_f32 - row_mean
    row_var = jnp.mean(centred * centred, axis=-1, keepdims=True)
    return (centred * lax.rsqrt(row_var + LN_EPS) * ln_gamma + ln_beta).astype(jnp.bfloat16)


def apply_rotary(vectors, cos_t, sin_t):
    as_f32 = vectors.astype(jnp.float32)
    lower_half = as_f32[..., :HALF_HEAD]
    upper_half = as_f32[..., HALF_HEAD:]
    return jnp.concatenate([lower_half * cos_t - upper_half * sin_t, upper_half * cos_t + lower_half * sin_t], axis=-1).astype(jnp.bfloat16)


def reference(x, ln_attn_gamma, ln_attn_beta, ln_mlp_gamma, ln_mlp_beta, w_qkv, w_out, w_up, w_down, k_cache, v_cache, positions):
    attn_in = layer_norm(x, ln_attn_gamma, ln_attn_beta)
    mlp_in = layer_norm(x, ln_mlp_gamma, ln_mlp_beta)
    qkv_rows = jnp.dot(attn_in, w_qkv.reshape(D, GROUPS * QKV_SLOTS * HEAD), preferred_element_type=jnp.float32).astype(jnp.bfloat16)
    qkv_rows = qkv_rows.reshape(BATCH, GROUPS, QKV_SLOTS, HEAD)
    inv_freq = ROPE_BASE ** (-2.0 * jnp.arange(HALF_HEAD, dtype=jnp.float32) / HEAD)
    angles = positions.astype(jnp.float32)[:, None] * inv_freq[None, :]
    cos_t = jnp.cos(angles)
    sin_t = jnp.sin(angles)
    queries = apply_rotary(qkv_rows[:, :, :QPG], cos_t[:, None, None, :], sin_t[:, None, None, :])
    new_key = apply_rotary(qkv_rows[:, :, QPG], cos_t[:, None, :], sin_t[:, None, :])
    new_value = qkv_rows[:, :, QPG + 1]
    slot_ids = jnp.arange(SEQ)
    write_mask = (slot_ids[None, :] == positions[:, None])[:, None, :, None]
    keys_all = jnp.where(write_mask, new_key[:, :, None, :], k_cache)
    values_all = jnp.where(write_mask, new_value[:, :, None, :], v_cache)
    valid_mask = slot_ids[None, :] <= positions[:, None]

    def attend_group(operands):
        q_grp, k_grp, v_grp = operands
        scores = jnp.einsum('bqh,bsh->bqs', q_grp.astype(jnp.float32), k_grp.astype(jnp.float32)) * SCORE_SCALE
        scores = jnp.where(valid_mask[:, None, :], scores, NEG_BIG)
        attn_probs = jax.nn.softmax(scores, axis=-1).astype(jnp.bfloat16)
        return jnp.einsum('bqs,bsh->bqh', attn_probs.astype(jnp.float32), v_grp.astype(jnp.float32)).astype(jnp.bfloat16)

    context = lax.map(attend_group, (jnp.moveaxis(queries, 1, 0), jnp.moveaxis(keys_all, 1, 0), jnp.moveaxis(values_all, 1, 0)))
    context = jnp.moveaxis(context, 0, 1).reshape(BATCH, GROUPS * QPG * HEAD)
    attn_out = jnp.dot(context, w_out.reshape(GROUPS * QPG * HEAD, D), preferred_element_type=jnp.float32)
    hidden = jax.nn.gelu(jnp.dot(mlp_in, w_up, preferred_element_type=jnp.float32), approximate=False).astype(jnp.bfloat16)
    mlp_out = jnp.dot(hidden, w_down, preferred_element_type=jnp.float32)
    layer_out = (x.astype(jnp.float32) + attn_out + mlp_out).astype(jnp.bfloat16)
    return (layer_out, keys_all, values_all)
```

```python
import functools
import math

import jax
import jax.numpy as jnp
from jax import lax
from jax.experimental import pallas as pl
from jax.experimental.pallas import tpu as pltpu
from jax.sharding import PartitionSpec as P

LN_EPS = 1e-5
ROPE_BASE = 10000.0
NEG_BIG = -1e30
MESH = pl.DeviceIdType.MESH
F32 = jnp.float32
BF16 = jnp.bfloat16

B = 256
D = 2048
S = 128
H = 128
G = 2
FL = 1024
R0 = 64
CH = 64
NG = 16
SCALE = H ** -0.5


def dot(a, b):
    return jnp.dot(a, b, preferred_element_type=F32)


def iota(shape, dim):
    return lax.broadcasted_iota(jnp.int32, shape, dim)


def build_queries(q_ref, row, qt_ref):
    stacked = jnp.concatenate([q_ref[pl.ds(row, CH), pl.ds(0, H)], q_ref[pl.ds(row, CH), pl.ds(H, H)]], axis=0)
    turned = stacked.T
    low = iota((H, 2 * CH), 1) < CH
    qt_ref[pl.ds(0, H), :] = jnp.where(low, turned, 0.0).astype(BF16)
    qt_ref[pl.ds(H, H), :] = jnp.where(low, 0.0, turned).astype(BF16)


def slot_mask(pos_s, row, slots):
    at = jnp.full((S, H), pos_s[row].astype(F32), F32).astype(BF16)
    return slots == at


def new_rows(new_ref, row):
    rows = pl.ds(row if isinstance(row, int) else pl.multiple_of(row, NG), NG)
    return [new_ref[rows, pl.ds(g * H, H)] for g in range(G)]


def patched(cache, mask, new, u):
    return jnp.where(mask, jnp.broadcast_to(new[u:u + 1], (S, H)).astype(BF16), cache)


def scores_of_group(pos_s, kn_ref, kbuf, qt_ref, acc, row, at, local):
    slots = iota((S, H), 0).astype(F32).astype(BF16)
    lane = iota((S, 2 * CH), 1) & (CH - 1)
    new = new_rows(kn_ref, row)
    for u in range(NG):
        mask = slot_mask(pos_s, row + u, slots)
        halves = []
        for g in range(G):
            k = patched(kbuf[at + u, g], mask, new[g], u)
            kbuf[at + u, g] = k
            halves.append(k)
        full = dot(jnp.concatenate(halves, axis=1), qt_ref[...])
        acc = jnp.where(lane == local + u, full, acc)
    return acc


def softmax_slots(acc, pos_v, chunk):
    row = pos_v[pl.ds(chunk // 2, 1), :]
    lane = iota((1, 2 * CH), 1)
    turned = pltpu.roll(row, CH, 1)
    at = jnp.where(lane < CH, row, turned) if chunk % 2 == 0 else jnp.where(lane < CH, turned, row)
    s = jnp.where(iota((S, 2 * CH), 0) <= at, acc * SCALE, NEG_BIG)
    e = jnp.exp(s - jnp.max(s, axis=0, keepdims=True))
    p = e / jnp.sum(e, axis=0, keepdims=True)
    return p.T.astype(BF16)


def context_of_group(pos_s, vn_ref, vbuf, p_ref, ctx_ref, row, at, local):
    slots = iota((S, H), 0).astype(F32).astype(BF16)
    rows16 = iota((NG, S), 0).astype(F32).astype(BF16)
    new = new_rows(vn_ref, row)
    total = [None, None]
    probs = [p_ref[pl.ds(pl.multiple_of(g * CH + local, NG), NG), :] for g in range(G)]
    zero = jnp.zeros((NG, S), BF16)
    for u in range(0, NG, 2):
        masks = [slot_mask(pos_s, row + u + w, slots) for w in range(2)]
        for g in range(G):
            vs, ps = [], []
            for w in range(2):
                v = patched(vbuf[at + u + w, g], masks[w], new[g], u + w)
                vbuf[at + u + w, g] = v
                vs.append(v)
                ps.append(jnp.where(rows16 == jnp.asarray(u + w, BF16), probs[g], zero))
            part = dot(jnp.concatenate(ps, axis=1), jnp.concatenate(vs, axis=0))
            total[g] = part if total[g] is None else total[g] + part
    for g in range(G):
        ctx_ref[pl.ds(pl.multiple_of(local, NG), NG), pl.ds(g * H, H)] = total[g].astype(BF16)


def local_kernel(x_h, ga_h, ba_h, gm_h, bm_h, wq_h, wo_h, wu_h, wd_h, k_h, v_h, pos_s, pos_h,
                 ko_h, vo_h, q_o, kn_o, vn_o, m_o, part_o,
                 x_v, ln_v, wq_v, w32_v, wqb_v, wo_v, wu_v, wd_v, kb, vb, pos_v, ain_v, min_v, cos_v, sin_v, h_v, qt_v, p_v, ctx_v, a_v,
                 sem_in, sem_k, sem_v, sem_ko, sem_vo):
    ngr = R0 // NG

    def rd(src, dst, i):
        c = pltpu.make_async_copy(src, dst, sem_in.at[i])
        c.start()
        return c

    c_pos = rd(pos_h, pos_v, 0)
    c_x = rd(x_h, x_v, 1)
    c_ln = [rd(r, ln_v.at[pl.ds(8 * i, 1)], 2 + i) for i, r in enumerate((ga_h, ba_h, gm_h, bm_h))]
    c_wq = [rd(wq_h.at[pl.ds(3072 * i, 3072)], wq_v.at[pl.ds(3072 * i, 3072)], 6 + i) for i in range(4)]

    def kcopy(i, a, b, sem):
        return pltpu.make_async_copy(a.at[pl.ds(NG * i, NG)], b.at[pl.ds(NG * i, NG)], sem.at[i])

    for i in range(ngr):
        kcopy(i, k_h, kb, sem_k).start()
    for i in range(ngr):
        kcopy(i, v_h, vb, sem_v).start()
    c_wo = rd(wo_h, wo_v, 10)
    c_wu = [rd(wu_h.at[pl.ds(1024 * i, 1024)], wu_v.at[pl.ds(1024 * i, 1024)], 11 + i) for i in range(2)]
    c_wd = [rd(wd_h.at[pl.ds(512 * i, 512)], wd_v.at[pl.ds(512 * i, 512)], 13 + i) for i in range(2)]

    c_pos.wait()
    lane = iota((S, H), 1)
    inv = jnp.exp((lane & (H // 2 - 1)).astype(F32) * (-2.0 * math.log(ROPE_BASE) / H))
    for i in range(2):
        at = jnp.broadcast_to(pos_v[pl.ds(i, 1), :].astype(F32), (S, H)).T
        ang = at * inv
        sn = jnp.sin(ang)
        cos_v[pl.ds(S * i, S), :] = jnp.cos(ang)
        sin_v[pl.ds(S * i, S), :] = jnp.where(lane < H // 2, -sn, sn)

    c_x.wait()
    for c in c_ln:
        c.wait()
    RB = 32

    @pl.loop(0, B // RB)
    def _(i):
        r = pl.ds(pl.multiple_of(i * RB, RB), RB)

        def tile(j):
            return x_v[r, pl.ds(128 * j, 128)].astype(F32)

        tot = tile(0)
        for j in range(1, 16):
            tot = tot + tile(j)
        mean = jnp.sum(tot, axis=-1, keepdims=True) * (1.0 / D)
        tot = jnp.zeros((RB, 128), F32)
        for j in range(16):
            d = tile(j) - mean
            tot = tot + d * d
        rs = lax.rsqrt(jnp.sum(tot, axis=-1, keepdims=True) * (1.0 / D) + LN_EPS)
        for j in range(16):
            cs = pl.ds(128 * j, 128)
            n = (tile(j) - mean) * rs
            ain_v[r, cs] = (n * ln_v[pl.ds(0, 1), cs] + ln_v[pl.ds(8, 1), cs]).astype(BF16)
            min_v[r, cs] = (n * ln_v[pl.ds(16, 1), cs] + ln_v[pl.ds(24, 1), cs]).astype(BF16)

    for c in c_wq:
        c.wait()

    @pl.loop(0, 16)
    def _(i):
        w32_v[...] = wq_v[pl.ds(pl.multiple_of(i * 768, 768), 768), :].astype(F32)
        for j in range(3):
            for g in range(G):
                wqb_v[pl.ds(pl.multiple_of(i * 128, 128), 128), pl.ds((g * 3 + j) * H, H)] = (
                    w32_v[pl.ds(2 * j + g, 128, stride=6), :].astype(BF16))

    def rotary(u, r):
        return u * cos_v[r, :] + pltpu.roll(u, H // 2, 1) * sin_v[r, :]

    for n in range(3):
        qkv = dot(ain_v[...], wqb_v[:, pl.ds(256 * n, 256)]).astype(BF16).astype(F32)
        for w in range(2):
            g, j = divmod(2 * n + w, 3)
            u = qkv[:, w * H:(w + 1) * H]
            dst = (q_o, kn_o, vn_o)[j]
            if j < 2:
                u = rotary(u, pl.ds(0, B)).astype(BF16).astype(F32)
            dst[:, pl.ds(g * H, H)] = u

    for c in range(R0 // CH):
        build_queries(q_o, c * CH, qt_v)
        acc = jnp.zeros((S, 2 * CH), F32)

        def score_step(j, acc, c=c):
            i = c * (CH // NG) + j
            kcopy(i, k_h, kb, sem_k).wait()
            return scores_of_group(pos_s, kn_o, kb, qt_v, acc, i * NG, i * NG, j * NG)

        acc = lax.fori_loop(0, CH // NG, score_step, acc)
        p_v[...] = softmax_slots(acc, pos_v, c)
        for j in range(CH // NG):
            kcopy(c * (CH // NG) + j, kb, ko_h, sem_ko).start()

        @pl.loop(0, CH // NG)
        def _(j, c=c):
            i = c * (CH // NG) + j
            kcopy(i, v_h, vb, sem_v).wait()
            context_of_group(pos_s, vn_o, vb, p_v, ctx_v, i * NG, i * NG, j * NG)

        if c == 0:
            c_wo.wait()
        for n in range(8):
            a_v[pl.ds(c * CH, CH), pl.ds(256 * n, 256)] = dot(ctx_v[...], wo_v[:, pl.ds(256 * n, 256)])
        for j in range(CH // NG):
            kcopy(c * (CH // NG) + j, vb, vo_h, sem_vo).start()

    for c in c_wu:
        c.wait()
    for n in range(4):
        u = dot(min_v[...], wu_v[:, pl.ds(256 * n, 256)])
        h_v[:, pl.ds(256 * n, 256)] = (0.5 * u * (1.0 + lax.erf(u * (2.0 ** -0.5)))).astype(BF16)
    for c in c_wd:
        c.wait()
    for n in range(8):
        cs = pl.ds(256 * n, 256)
        m_o[:, cs] = dot(h_v[...], wd_v[:, cs])
        part_o[:, cs] = (a_v[:, cs] + m_o[pl.ds(0, R0), cs]).astype(BF16)

    for i in range(ngr):
        kcopy(i, kb, ko_h, sem_ko).wait()
        kcopy(i, vb, vo_h, sem_vo).wait()


def reduce_kernel(x_h, wo_h, k_h, v_h, q_i, kn_i, vn_i, m_i, part_i, pos_s, pos_i,
                  k2, v2, out_o,
                  x_v, wo_v, qt_v, p_v, ctx_v, part_v, d2_v, sum_v, rs_v, gat_v,
                  sem_in, sem_k, sem_v, s_d, r_d, s_rs, r_rs, s_ag, r_ag, s_e, r_e):
    tp = lax.axis_index("tp")
    core = tp % 2
    chip = tp // 2
    nch = B // CH
    first = R0 // CH
    ngr = (B - R0) // NG
    HR = CH // 2
    QC = D // 4

    def kcopy(i, a, b, sem):
        return pltpu.make_async_copy(a.at[pl.ds(R0 + NG * i, NG)], b.at[pl.ds(NG * i, NG)], sem.at[i])

    per = CH // NG
    for c in range(nch - first):
        for i in range(per):
            kcopy(c * per + i, k_h, k2, sem_k).start()
        for i in range(per):
            kcopy(c * per + i, v_h, v2, sem_v).start()
        if c == 0:
            c_wo = pltpu.make_async_copy(wo_h, wo_v, sem_in.at[0])
            c_wo.start()
            c_x = pltpu.make_async_copy(x_h, x_v, sem_in.at[1])
            c_x.start()

    sib = tp + 1 - 2 * core
    peers = []
    for k in range(1, 4):
        chip_k = (chip // 2 + k // 2) % 2 * 2 + (chip % 2 + k % 2) % 2
        peers.append((chip_k, chip_k * 2 + core))

    barrier = pltpu.get_barrier_semaphore()
    for t in [sib] + [p for _, p in peers]:
        pl.semaphore_signal(barrier, inc=1, device_id={"tp": t}, device_id_type=MESH)
    pl.semaphore_wait(barrier, 4)

    def part_of(c):
        return part_i.at[pl.ds(c * CH, CH)] if c < first else part_v.at[pl.ds((c - first) * CH, CH)]

    my_rows = pl.ds(pl.multiple_of(core * HR, HR), HR)
    sib_rows = pl.ds(pl.multiple_of((1 - core) * HR, HR), HR)
    my_cols = pl.ds(pl.multiple_of(chip * QC, QC), QC)

    def remote(src, dst, s, r, t):
        return pltpu.make_async_remote_copy(src_ref=src, dst_ref=dst, send_sem=s, recv_sem=r, device_id={"tp": t}, device_id_type=MESH)

    def a_copy(c):
        return remote(part_of(c).at[sib_rows], d2_v.at[c], s_d.at[c], r_d.at[c], sib)

    def b_copies(c):
        return [remote(sum_v.at[c, :, pl.ds(pl.multiple_of(ck * QC, QC), QC)], rs_v.at[c, k], s_rs.at[c, k], r_rs.at[c, k], t)
                for k, (ck, t) in enumerate(peers)]

    def out_rows(c):
        return pl.ds(pl.multiple_of(c * CH + core * HR, HR), HR)

    def c_copies(c):
        piece = gat_v.at[out_rows(c), my_cols]
        return [remote(piece, piece, s_ag.at[c, k], r_ag.at[c, k], t) for k, (_, t) in enumerate(peers)]

    def d_copy(c):
        rows = gat_v.at[out_rows(c)]
        return remote(rows, rows, s_e.at[c], r_e.at[c], sib)

    def step_a(c):
        a_copy(c).start()

    def step_b(c):
        a_copy(c).wait_recv()
        own = part_of(c)
        sum_v[c] = (own[my_rows, :].astype(F32) + d2_v[c].astype(F32)).astype(BF16)
        for cp in b_copies(c):
            cp.start()

    def step_c(c):
        tot = sum_v[c, :, my_cols].astype(F32)
        for k, cp in enumerate(b_copies(c)):
            cp.wait_recv()
            tot = tot + rs_v[c, k].astype(F32)
        tot = tot + x_v[out_rows(c), my_cols].astype(F32)
        gat_v[out_rows(c), my_cols] = tot.astype(BF16)
        for cp in c_copies(c):
            cp.start()

    def step_d(c):
        for cp in c_copies(c):
            cp.wait_recv()
        d_copy(c).start()

    def attend_scores(c):
        build_queries(q_i, c * CH, qt_v)
        acc = jnp.zeros((S, 2 * CH), F32)

        def score_step(j, acc):
            i = (c - first) * per + j
            kcopy(i, k_h, k2, sem_k).wait()
            return scores_of_group(pos_s, kn_i, k2, qt_v, acc, R0 + i * NG, i * NG, j * NG)

        acc = lax.fori_loop(0, per, score_step, acc)
        p_v[...] = softmax_slots(acc, pos_i, c)

    def attend_context(c):
        @pl.loop(0, per)
        def _(j):
            i = (c - first) * per + j
            kcopy(i, v_h, v2, sem_v).wait()
            context_of_group(pos_s, vn_i, v2, p_v, ctx_v, R0 + i * NG, i * NG, j * NG)

        if c == first:
            c_wo.wait()
            c_x.wait()
        for n in range(8):
            cs = pl.ds(256 * n, 256)
            part_v[pl.ds((c - first) * CH, CH), cs] = (dot(ctx_v[...], wo_v[:, cs]) + m_i[pl.ds(c * CH, CH), cs]).astype(BF16)

    step_a(0)
    attend_scores(1)
    step_b(0)
    attend_context(1)
    step_a(1)
    attend_scores(2)
    step_b(1)
    attend_context(2)
    step_a(2)
    step_c(0)
    attend_scores(3)
    step_b(2)
    attend_context(3)
    step_a(3)
    step_c(1)
    step_d(0)
    step_b(3)
    step_c(2)
    step_d(1)
    step_c(3)
    step_d(2)
    step_d(3)
    for c in range(nch):
        a_copy(c).wait_send()
        for cp in b_copies(c):
            cp.wait_send()
        for cp in c_copies(c):
            cp.wait_send()
        d_copy(c).wait()
    out_o[...] = gat_v[...]


def write_kernel(k_i, v_i, o_i, k0_h, v0_h, ko_h, vo_h, o_h, sem):
    n = (B - R0) // NG // 2
    copies = []
    for i in range(n):
        rows = pl.ds(2 * NG * i, 2 * NG)
        dst = pl.ds(R0 + 2 * NG * i, 2 * NG)
        copies.append(pltpu.make_async_copy(k_i.at[rows], ko_h.at[dst], sem.at[2 * i]))
        copies.append(pltpu.make_async_copy(v_i.at[rows], vo_h.at[dst], sem.at[2 * i + 1]))
    copies.append(pltpu.make_async_copy(o_i, o_h, sem.at[2 * n]))
    for c in copies:
        c.start()
    for c in copies:
        c.wait()


def solution(mesh):
    row_spec = P('dp', None)
    vec_spec = P(None)
    cache_spec = P('dp', 'tp', None, None)
    vm = pl.BlockSpec(memory_space=pltpu.VMEM)
    sm = pl.BlockSpec(memory_space=pltpu.SMEM)
    anyspace = pl.BlockSpec(memory_space=pl.ANY)
    dma = pltpu.SemaphoreType.DMA
    MIB = 1024 * 1024

    def hbm(t):
        return pltpu.with_memory_space_constraint(t, pltpu.HBM)

    def device_step(x, ln_attn_gamma, ln_attn_beta, ln_mlp_gamma, ln_mlp_beta, w_qkv, w_out, w_up, w_down, k_cache, v_cache, positions):
        wq = w_qkv.transpose(0, 2, 1, 3).reshape(D * 3 * G, H)
        wo = w_out.reshape(G * H, D)
        pos2 = positions.reshape(2, 128)
        cache = jax.ShapeDtypeStruct((B, G, S, H), BF16)
        NR = B - R0
        k0, v0, q, kn, vn, m, part = pl.pallas_call(
            local_kernel,
            out_shape=(cache, cache) + (pltpu.VMEM((B, G * H), F32),) * 3 + (pltpu.VMEM((B, D), F32), pltpu.VMEM((R0, D), BF16)),
            in_specs=[anyspace] * 11 + [sm, anyspace],
            out_specs=(anyspace, anyspace) + (vm,) * 5,
            scratch_shapes=[
                pltpu.VMEM((B, D), BF16), pltpu.VMEM((32, D), F32), pltpu.VMEM((D * 3 * G, H), BF16), pltpu.VMEM((768, H), F32),
                pltpu.VMEM((D, 768), BF16), pltpu.VMEM((G * H, D), BF16), pltpu.VMEM((D, FL), BF16), pltpu.VMEM((FL, D), BF16),
                pltpu.VMEM((R0, G, S, H), BF16), pltpu.VMEM((R0, G, S, H), BF16), pltpu.VMEM((2, 128), jnp.int32),
                pltpu.VMEM((B, D), BF16), pltpu.VMEM((B, D), BF16), pltpu.VMEM((B, H), F32), pltpu.VMEM((B, H), F32),
                pltpu.VMEM((B, FL), BF16), pltpu.VMEM((G * H, 2 * CH), BF16), pltpu.VMEM((2 * CH, S), BF16), pltpu.VMEM((CH, G * H), BF16),
                pltpu.VMEM((R0, D), F32),
                dma((15,)), dma((R0 // NG,)), dma((R0 // NG,)), dma((R0 // NG,)), dma((R0 // NG,)),
            ],
            compiler_params=pltpu.CompilerParams(vmem_limit_bytes=40 * MIB),
            name="local_part",
        )(hbm(x), *[hbm(t.reshape(1, D)) for t in (ln_attn_gamma, ln_attn_beta, ln_mlp_gamma, ln_mlp_beta)],
          hbm(wq), hbm(wo), hbm(w_up), hbm(w_down), hbm(k_cache), hbm(v_cache), positions, hbm(pos2))

        nch = B // CH
        k2, v2, o = pl.pallas_call(
            reduce_kernel,
            out_shape=(pltpu.VMEM((NR, G, S, H), BF16), pltpu.VMEM((NR, G, S, H), BF16), pltpu.VMEM((B, D), BF16)),
            in_specs=[anyspace] * 4 + [vm] * 5 + [sm, vm],
            out_specs=(vm,) * 3,
            scratch_shapes=[
                pltpu.VMEM((B, D), BF16), pltpu.VMEM((G * H, D), BF16), pltpu.VMEM((G * H, 2 * CH), BF16), pltpu.VMEM((2 * CH, S), BF16),
                pltpu.VMEM((CH, G * H), BF16), pltpu.VMEM((NR, D), BF16), pltpu.VMEM((nch, CH // 2, D), BF16),
                pltpu.VMEM((nch, CH // 2, D), BF16), pltpu.VMEM((nch, 3, CH // 2, D // 4), BF16), pltpu.VMEM((B, D), BF16),
                dma((2,)), dma((NR // NG,)), dma((NR // NG,)),
                dma((nch,)), dma((nch,)), dma((nch, 3)), dma((nch, 3)), dma((nch, 3)), dma((nch, 3)), dma((nch,)), dma((nch,)),
            ],
            compiler_params=pltpu.CompilerParams(vmem_limit_bytes=16 * MIB, collective_id=0, has_side_effects=True),
            name="reduce_part",
        )(hbm(x), hbm(wo), hbm(k_cache), hbm(v_cache), q, kn, vn, m, part, positions, pos2)

        kf, vf, out = pl.pallas_call(
            write_kernel,
            out_shape=(cache, cache, jax.ShapeDtypeStruct((B, D), BF16)),
            in_specs=[vm] * 3 + [anyspace] * 2,
            out_specs=(anyspace,) * 3,
            scratch_shapes=[dma((NR // NG + 1,))],
            input_output_aliases={3: 0, 4: 1},
            compiler_params=pltpu.CompilerParams(vmem_limit_bytes=4 * MIB),
            name="write_part",
        )(k2, v2, o, k0, v0)
        return out, kf, vf

    return jax.shard_map(device_step, mesh=mesh, in_specs=(row_spec, vec_spec, vec_spec, vec_spec, vec_spec, P(None, 'tp', None, None), P('tp', None, None, None), P(None, 'tp'), P('tp', None), cache_spec, cache_spec, P('dp')), out_specs=(row_spec, cache_spec, cache_spec), check_vma=False)
```

```python
import functools
import math

import jax
import jax.numpy as jnp
from jax import lax
from jax.experimental import pallas as pl
from jax.experimental.pallas import tpu as pltpu
from jax.sharding import PartitionSpec as P

LN_EPS = 1e-5
ROPE_BASE = 10000.0
NEG_BIG = -1e30
MESH = pl.DeviceIdType.MESH
F32 = jnp.float32
BF16 = jnp.bfloat16

B = 256
D = 2048
S = 128
H = 128
G = 2
FL = 1024
R0 = 64
CH = 64
NG = 16
GI = 2
SCALE = H ** -0.5
PER = CH // NG


def dot(a, b):
    return jnp.dot(a, b, preferred_element_type=F32)


def iota(shape, dim):
    return lax.broadcasted_iota(jnp.int32, shape, dim)


def build_queries(q_ref, row, qt_ref):
    stacked = jnp.concatenate([q_ref[pl.ds(row, CH), pl.ds(0, H)], q_ref[pl.ds(row, CH), pl.ds(H, H)]], axis=0)
    turned = stacked.T
    low = iota((H, 2 * CH), 1) < CH
    qt_ref[pl.ds(0, H), :] = jnp.where(low, turned, 0.0).astype(BF16)
    qt_ref[pl.ds(H, H), :] = jnp.where(low, 0.0, turned).astype(BF16)


def add_rows(buf, new_ref, pos_s, row, at):
    rows = pl.ds(row if isinstance(row, int) else pl.multiple_of(row, NG), NG)
    new = [new_ref[rows, pl.ds(g * H, H)] for g in range(G)]
    inside = iota((NG, H), 0).astype(F32).astype(BF16)
    for u in range(NG):
        pos = pos_s[row + u]
        start = pl.multiple_of(lax.shift_left(lax.shift_right_logical(pos, 4), 4), NG)
        mask = inside == jnp.full((NG, H), (pos - start).astype(F32), F32).astype(BF16)
        for g in range(G):
            tile = buf.at[at + u, g, pl.ds(start, NG), :]
            tile[...] = jnp.where(mask, jnp.broadcast_to(new[g][u:u + 1], (NG, H)).astype(BF16), tile[...])


def scores_of_group(kbuf, qt_ref, acc, at, local):
    lane = iota((S, 2 * CH), 1) & (CH - 1)
    for u in range(NG):
        keys = jnp.concatenate([kbuf[at + u, g] for g in range(G)], axis=1)
        acc = jnp.where(lane == local + u, dot(keys, qt_ref[...]), acc)
    return acc


def attend_scores(c, at, wait, also, kbuf, q_ref, kn_ref, pos_v, qt_v, p_v, pn_v):
    build_queries(q_ref, c * CH, qt_v)
    rows = pl.ds(c * CH, CH)
    with_new = jnp.concatenate([q_ref[rows, pl.ds(g * H, H)] * kn_ref[rows, pl.ds(g * H, H)] for g in range(G)], axis=0)
    s_new = jnp.sum(with_new.T, axis=0, keepdims=True)
    new_at = pos_columns(pos_v, c)

    def step(j, acc):
        for w in range(GI):
            wait(j * GI + w)
        for w in range(GI):
            i = j * GI + w
            acc = scores_of_group(kbuf, qt_v, acc, at + i * NG, i * NG)
            also(i)
        return acc

    acc = lax.fori_loop(0, CH // NG // GI, step, jnp.zeros((S, 2 * CH), F32))
    slot = iota((S, 2 * CH), 0)
    s = jnp.where(slot < new_at, acc * SCALE, jnp.where(slot == new_at, s_new * SCALE, NEG_BIG))
    p = softmax_slots(s).astype(BF16).astype(F32)
    p_v[...] = jnp.where(slot == new_at, 0.0, p).T.astype(BF16)
    p_new = jnp.sum(jnp.where(slot == new_at, p, 0.0), axis=0, keepdims=True)
    pn_v[...] = jnp.broadcast_to(p_new, (2 * CH, H)).T


def attend_context(c, at, lo, hi, wait, also, vbuf, vn_ref, p_v, pn_v, ctx_v):
    @pl.loop(0, (hi - lo) // GI)
    def _(j):
        for w in range(GI):
            wait(lo + j * GI + w)
        for w in range(GI):
            i = lo + j * GI + w
            ctx = context_of_group(vbuf, p_v, at + i * NG, i * NG)
            rows = pl.ds(pl.multiple_of(c * CH + i * NG, NG), NG)
            for g in range(G):
                new = pn_v[pl.ds(pl.multiple_of(g * CH + i * NG, NG), NG), :] * vn_ref[rows, pl.ds(g * H, H)]
                ctx_v[pl.ds(pl.multiple_of(i * NG, NG), NG), pl.ds(g * H, H)] = (ctx[g] + new).astype(BF16)
            also(i)


def pos_columns(pos_v, chunk):
    row = pos_v[pl.ds(chunk // 2, 1), :]
    lane = iota((1, 2 * CH), 1)
    turned = pltpu.roll(row, CH, 1)
    return jnp.where(lane < CH, row, turned) if chunk % 2 == 0 else jnp.where(lane < CH, turned, row)


def softmax_slots(s):
    e = jnp.exp(s - jnp.max(s, axis=0, keepdims=True))
    return e / jnp.sum(e, axis=0, keepdims=True)


def context_of_group(vbuf, p_ref, at, local):
    rows16 = iota((NG, S), 0).astype(F32).astype(BF16)
    zero = jnp.zeros((NG, S), BF16)
    total = []
    for g in range(G):
        probs = p_ref[pl.ds(pl.multiple_of(g * CH + local, NG), NG), :]
        tot = None
        for u in range(0, NG, 2):
            ps = [jnp.where(rows16 == jnp.asarray(u + w, BF16), probs, zero) for w in range(2)]
            vs = [vbuf[at + u + w, g] for w in range(2)]
            part = dot(jnp.concatenate(ps, axis=1), jnp.concatenate(vs, axis=0))
            tot = part if tot is None else tot + part
        total.append(tot)
    return total


def local_kernel(x_h, ga_h, ba_h, gm_h, bm_h, wq_h, wo_h, wu_h, wd_h, k_h, v_h, pos_s, pos_h,
                 ko_h, vo_h, q_o, kn_o, vn_o, m_o, part_o, x_v, wo_v, kp_o,
                 ln_v, wq_v, w32_v, wqb_v, wu_v, wd_v, kb, vb, pos_v, ain_v, min_v, cos_v, sin_v, h_v, qt_v, p_v, pn_v, ctx_v, a_v,
                 sem_in, sem_k, sem_v, sem_ko, sem_vo, sem_kp):
    ngr = R0 // NG

    def rd(src, dst, i):
        c = pltpu.make_async_copy(src, dst, sem_in.at[i])
        c.start()
        return c

    c_pos = rd(pos_h, pos_v, 0)
    c_x = [rd(x_h.at[pl.ds(64 * i, 64)], x_v.at[pl.ds(64 * i, 64)], 15 + i) for i in range(4)]
    c_ln = [rd(r, ln_v.at[pl.ds(8 * i, 1)], 2 + i) for i, r in enumerate((ga_h, ba_h, gm_h, bm_h))]
    c_wq = [rd(wq_h.at[pl.ds(3072 * i, 3072)], wq_v.at[pl.ds(3072 * i, 3072)], 6 + i) for i in range(4)]

    def kcopy(i, a, b, sem):
        return pltpu.make_async_copy(a.at[pl.ds(NG * i, NG)], b.at[pl.ds(NG * i, NG)], sem.at[i])

    kp_copies = [pltpu.make_async_copy(k_h.at[pl.ds(R0 + NG * i, NG)], kp_o.at[pl.ds(NG * i, NG)], sem_kp.at[i]) for i in range(PER)]

    c_pos.wait()
    lane = iota((S, H), 1)
    inv = jnp.exp((lane & (H // 2 - 1)).astype(F32) * (-2.0 * math.log(ROPE_BASE) / H))
    for i in range(2):
        at = jnp.broadcast_to(pos_v[pl.ds(i, 1), :].astype(F32), (S, H)).T
        ang = at * inv
        sn = jnp.sin(ang)
        cos_v[pl.ds(S * i, S), :] = jnp.cos(ang)
        sin_v[pl.ds(S * i, S), :] = jnp.where(lane < H // 2, -sn, sn)

    for c in c_ln + c_x:
        c.wait()
    for i in range(PER):
        kcopy(i, k_h, kb, sem_k).start()
    RB = 16
    NB = 4

    @pl.loop(0, B // (RB * NB))
    def _(i):
        rows = [pl.ds(pl.multiple_of(i * (RB * NB) + RB * w, RB), RB) for w in range(NB)]

        def tile(r, j):
            return x_v[r, pl.ds(128 * j, 128)].astype(F32)

        means, scales = [], []
        for r in rows:
            tot = tile(r, 0)
            for j in range(1, 16):
                tot = tot + tile(r, j)
            means.append(jnp.sum(tot, axis=-1, keepdims=True) * (1.0 / D))
        for r, mean in zip(rows, means):
            tot = jnp.zeros((RB, 128), F32)
            for j in range(16):
                d = tile(r, j) - mean
                tot = tot + d * d
            scales.append(lax.rsqrt(jnp.sum(tot, axis=-1, keepdims=True) * (1.0 / D) + LN_EPS))
        for r, mean, rs in zip(rows, means, scales):
            for j in range(16):
                cs = pl.ds(128 * j, 128)
                n = (tile(r, j) - mean) * rs
                ain_v[r, cs] = (n * ln_v[pl.ds(0, 1), cs] + ln_v[pl.ds(8, 1), cs]).astype(BF16)
                min_v[r, cs] = (n * ln_v[pl.ds(16, 1), cs] + ln_v[pl.ds(24, 1), cs]).astype(BF16)

    for c in c_wq:
        c.wait()
    for i in range(PER):
        kcopy(i, v_h, vb, sem_v).start()
    c_wo = rd(wo_h, wo_v, 10)
    c_wu = [rd(wu_h.at[pl.ds(1024 * i, 1024)], wu_v.at[pl.ds(1024 * i, 1024)], 11 + i) for i in range(2)]

    @pl.loop(0, 16)
    def _(i):
        w32_v[...] = wq_v[pl.ds(pl.multiple_of(i * 768, 768), 768), :].astype(F32)
        for j in range(3):
            for g in range(G):
                wqb_v[pl.ds(pl.multiple_of(i * 128, 128), 128), pl.ds((g * 3 + j) * H, H)] = (
                    w32_v[pl.ds(2 * j + g, 128, stride=6), :].astype(BF16))

    def rotary(u, r):
        return u * cos_v[r, :] + pltpu.roll(u, H // 2, 1) * sin_v[r, :]

    for n in range(3):
        qkv = dot(ain_v[...], wqb_v[:, pl.ds(256 * n, 256)]).astype(BF16).astype(F32)
        for w in range(2):
            g, j = divmod(2 * n + w, 3)
            u = qkv[:, w * H:(w + 1) * H]
            dst = (q_o, kn_o, vn_o)[j]
            if j < 2:
                u = rotary(u, pl.ds(0, B)).astype(BF16).astype(F32)
            dst[:, pl.ds(g * H, H)] = u

    for c in range(R0 // CH):
        c_wd = [rd(wd_h.at[pl.ds(512 * i, 512)], wd_v.at[pl.ds(512 * i, 512)], 13 + i) for i in range(2)]
        base = c * CH

        def wait_k(i, c=c):
            kcopy(c * PER + i, k_h, kb, sem_k).wait()

        def wait_v(i, c=c):
            kcopy(c * PER + i, v_h, vb, sem_v).wait()

        def old_v(i, c=c):
            if c > 0:
                add_rows(vb, vn_o, pos_s, base - CH + i * NG, base - CH + i * NG)

        def add_k(i):
            add_rows(kb, kn_o, pos_s, base + i * NG, base + i * NG)

        attend_scores(c, base, wait_k, old_v, kb, q_o, kn_o, pos_v, qt_v, p_v, pn_v)
        if c > 0:
            for j in range(PER):
                kcopy((c - 1) * PER + j, vb, vo_h, sem_vo).start()
        for cp in kp_copies:
            cp.start()
        attend_context(c, base, 0, PER, wait_v, add_k, vb, vn_o, p_v, pn_v, ctx_v)
        if c == 0:
            c_wo.wait()
        for n in range(8):
            a_v[pl.ds(base, CH), pl.ds(256 * n, 256)] = dot(ctx_v[...], wo_v[:, pl.ds(256 * n, 256)])
        for j in range(PER):
            kcopy(c * PER + j, kb, ko_h, sem_ko).start()

    for c in c_wu:
        c.wait()
    for n in range(4):
        u = dot(min_v[...], wu_v[:, pl.ds(256 * n, 256)])
        h_v[:, pl.ds(256 * n, 256)] = (0.5 * u * (1.0 + lax.erf(u * (2.0 ** -0.5)))).astype(BF16)
        add_rows(vb, vn_o, pos_s, R0 - CH + n * NG, R0 - CH + n * NG)
    for j in range(PER):
        kcopy(R0 // NG - PER + j, vb, vo_h, sem_vo).start()
    for c in c_wd:
        c.wait()
    for n in range(8):
        cs = pl.ds(256 * n, 256)
        m_o[:, cs] = dot(h_v[...], wd_v[:, cs])
        part_o[:, cs] = (a_v[:, cs] + m_o[pl.ds(0, R0), cs]).astype(BF16)

    for cp in kp_copies:
        cp.wait()
    for i in range(ngr):
        kcopy(i, kb, ko_h, sem_ko).wait()
        kcopy(i, vb, vo_h, sem_vo).wait()


PARTS = ((0, 64), (64, 64), (128, 64), (192, 32), (224, 32))


def reduce_kernel(k_h, v_h, q_i, kn_i, vn_i, m_i, part_i, x_v, wo_v, kp_i, pos_i,
                  k2, v2, out_o,
                  qt_v, p_v, pn_v, ctx_v, part_v, d2_v, sum_v, rs_v, gat_v,
                  sem_k, sem_v, s_d, r_d, s_rs, r_rs, s_ag, r_ag, s_e, r_e):
    tp = lax.axis_index("tp")
    core = tp % 2
    chip = tp // 2
    first = R0 // CH
    per = CH // NG
    QC = D // 4

    def kcopy(i):
        return pltpu.make_async_copy(k_h.at[pl.ds(R0 + CH + NG * i, NG)], k2.at[pl.ds(NG * i, NG)], sem_k.at[i])

    def vcopy(i):
        return pltpu.make_async_copy(v_h.at[pl.ds(R0 + NG * i, NG)], v2.at[pl.ds(NG * i, NG)], sem_v.at[i])

    def issue_k(c):
        for i in range(per):
            kcopy((c - first - 1) * per + i).start()

    def issue_v(c):
        for i in range(per):
            vcopy((c - first) * per + i).start()

    issue_v(1)
    issue_k(2)

    sib = tp + 1 - 2 * core
    peers = []
    for k in range(1, 4):
        chip_k = (chip // 2 + k // 2) % 2 * 2 + (chip % 2 + k % 2) % 2
        peers.append((chip_k, chip_k * 2 + core))

    barrier = pltpu.get_barrier_semaphore()
    for t in [sib] + [p for _, p in peers]:
        pl.semaphore_signal(barrier, inc=1, device_id={"tp": t}, device_id_type=MESH)
    my_cols = pl.ds(pl.multiple_of(chip * QC, QC), QC)

    def remote(src, dst, s, r, t):
        return pltpu.make_async_remote_copy(src_ref=src, dst_ref=dst, send_sem=s, recv_sem=r, device_id={"tp": t}, device_id_type=MESH)

    def part_of(c, which):
        start, n = PARTS[c]
        ref, base = (part_i, start) if start < R0 else (part_v, start - R0)
        return ref.at[pl.ds(pl.multiple_of(base + which * (n // 2), NG), n // 2)]

    def half(c):
        start, n = PARTS[c]
        return pl.ds(start // 2, n // 2)

    def out_rows(c):
        start, n = PARTS[c]
        return pl.ds(pl.multiple_of(start + core * (n // 2), NG), n // 2)

    def a_copy(c):
        return remote(part_of(c, 1 - core), d2_v.at[half(c)], s_d.at[c], r_d.at[c], sib)

    def b_copies(c):
        return [remote(sum_v.at[half(c), pl.ds(pl.multiple_of(ck * QC, QC), QC)], rs_v.at[k, half(c)], s_rs.at[c, k], r_rs.at[c, k], t)
                for k, (ck, t) in enumerate(peers)]

    def c_copies(c):
        piece = gat_v.at[out_rows(c), my_cols]
        return [remote(piece, piece, s_ag.at[c, k], r_ag.at[c, k], t) for k, (_, t) in enumerate(peers)]

    def d_copy(c):
        rows = gat_v.at[out_rows(c)]
        return remote(rows, rows, s_e.at[c], r_e.at[c], sib)

    def step_a(c):
        a_copy(c).start()

    def step_b(c):
        a_copy(c).wait_recv()
        sum_v[half(c)] = (part_of(c, core)[...].astype(F32) + d2_v[half(c)].astype(F32)).astype(BF16)
        for cp in b_copies(c):
            cp.start()

    def step_c(c):
        tot = sum_v[half(c), my_cols].astype(F32) + x_v[out_rows(c), my_cols].astype(F32)
        for k, cp in enumerate(b_copies(c)):
            cp.wait_recv()
            tot = tot + rs_v[k, half(c)].astype(F32)
        gat_v[out_rows(c), my_cols] = tot.astype(BF16)
        for cp in c_copies(c):
            cp.start()

    def step_d(c):
        for cp in c_copies(c):
            cp.wait_recv()
        d_copy(c).start()

    def nothing(i):
        pass

    def scores(c):
        if c == first:
            attend_scores(c, 0, nothing, nothing, kp_i, q_i, kn_i, pos_i, qt_v, p_v, pn_v)
        else:
            at = (c - first - 1) * per
            attend_scores(c, at * NG, lambda i: kcopy(at + i).wait(), nothing, k2, q_i, kn_i, pos_i, qt_v, p_v, pn_v)

    def context(c, lo, hi):
        at = (c - first) * CH
        attend_context(c, at, lo, hi, lambda i: vcopy((c - first) * per + i).wait(), nothing, v2, vn_i, p_v, pn_v, ctx_v)
        n = (hi - lo) * NG
        for k in range(8):
            cs = pl.ds(256 * k, 256)
            part_v[pl.ds(at + lo * NG, n), cs] = (
                dot(ctx_v[pl.ds(lo * NG, n), :], wo_v[:, cs]) + m_i[pl.ds(c * CH + lo * NG, n), cs]).astype(BF16)

    pl.semaphore_wait(barrier, 4)
    step_a(0)
    scores(1)
    step_b(0)
    issue_v(2)
    context(1, 0, per)
    step_a(1)
    issue_k(3)
    scores(2)
    step_b(1)
    step_c(0)
    issue_v(3)
    context(2, 0, per)
    step_a(2)
    scores(3)
    step_b(2)
    context(3, 0, per // 2)
    step_a(3)
    step_c(1)
    context(3, per // 2, per)
    step_a(4)
    step_b(3)
    step_b(4)
    step_d(0)
    step_c(2)
    step_d(1)
    step_c(3)
    step_c(4)
    step_d(2)
    step_d(3)
    step_d(4)
    for c in range(len(PARTS)):
        a_copy(c).wait_send()
        for cp in b_copies(c):
            cp.wait_send()
        for cp in c_copies(c):
            cp.wait_send()
        d_copy(c).wait()
    out_o[...] = gat_v[...]


def write_kernel(kp_i, k_i, v_i, o_i, kn_i, vn_i, pos_s, k0_h, v0_h, kp3, k3, v3, ko_h, vo_h, o_h, sem):
    n = (B - R0) // NG
    c_out = pltpu.make_async_copy(o_i, o_h, sem.at[2 * n])
    c_out.start()

    def copy(src, dst, i, k):
        return pltpu.make_async_copy(src.at[pl.ds(NG * i, NG)], dst.at[pl.ds(R0 + NG * k, NG)], sem.at[k if dst is ko_h else n + k])

    for src, dst, new, first, count in ((kp3, ko_h, kn_i, 0, PER), (v3, vo_h, vn_i, 0, n), (k3, ko_h, kn_i, PER, n - PER)):
        @pl.loop(0, count)
        def _(i, src=src, dst=dst, new=new, first=first):
            add_rows(src, new, pos_s, R0 + (first + i) * NG, i * NG)

            @pl.when(i > 0)
            def _():
                copy(src, dst, i - 1, first + i - 1).start()

        copy(src, dst, count - 1, first + count - 1).start()

    for src, dst, first, count in ((kp3, ko_h, 0, PER), (v3, vo_h, 0, n), (k3, ko_h, PER, n - PER)):
        @pl.loop(0, count)
        def _(i, src=src, dst=dst, first=first):
            copy(src, dst, i, first + i).wait()

    c_out.wait()


def solution(mesh):
    row_spec = P('dp', None)
    vec_spec = P(None)
    cache_spec = P('dp', 'tp', None, None)
    vm = pl.BlockSpec(memory_space=pltpu.VMEM)
    sm = pl.BlockSpec(memory_space=pltpu.SMEM)
    anyspace = pl.BlockSpec(memory_space=pl.ANY)
    dma = pltpu.SemaphoreType.DMA
    MIB = 1024 * 1024

    def hbm(t):
        return pltpu.with_memory_space_constraint(t, pltpu.HBM)

    def device_step(x, ln_attn_gamma, ln_attn_beta, ln_mlp_gamma, ln_mlp_beta, w_qkv, w_out, w_up, w_down, k_cache, v_cache, positions):
        wq = w_qkv.transpose(0, 2, 1, 3).reshape(D * 3 * G, H)
        wo = w_out.reshape(G * H, D)
        pos2 = positions.reshape(2, 128)
        cache = jax.ShapeDtypeStruct((B, G, S, H), BF16)
        NR = B - R0
        k0, v0, q, kn, vn, m, part, xv, wov, kp = pl.pallas_call(
            local_kernel,
            out_shape=(cache, cache) + (pltpu.VMEM((B, G * H), F32),) * 3 + (pltpu.VMEM((B, D), F32), pltpu.VMEM((R0, D), BF16), pltpu.VMEM((B, D), BF16),
                                                                              pltpu.VMEM((G * H, D), BF16), pltpu.VMEM((CH, G, S, H), BF16)),
            in_specs=[anyspace] * 11 + [sm, anyspace],
            out_specs=(anyspace, anyspace) + (vm,) * 8,
            scratch_shapes=[
                pltpu.VMEM((32, D), F32), pltpu.VMEM((D * 3 * G, H), BF16), pltpu.VMEM((768, H), F32),
                pltpu.VMEM((D, 768), BF16), pltpu.VMEM((D, FL), BF16), pltpu.VMEM((FL, D), BF16),
                pltpu.VMEM((R0, G, S, H), BF16), pltpu.VMEM((R0, G, S, H), BF16), pltpu.VMEM((2, 128), jnp.int32),
                pltpu.VMEM((B, D), BF16), pltpu.VMEM((B, D), BF16), pltpu.VMEM((B, H), F32), pltpu.VMEM((B, H), F32),
                pltpu.VMEM((B, FL), BF16), pltpu.VMEM((G * H, 2 * CH), BF16), pltpu.VMEM((2 * CH, S), BF16), pltpu.VMEM((2 * CH, H), F32),
                pltpu.VMEM((CH, G * H), BF16), pltpu.VMEM((R0, D), F32),
                dma((19,)), dma((R0 // NG,)), dma((R0 // NG,)), dma((R0 // NG,)), dma((R0 // NG,)), dma((PER,)),
            ],
            compiler_params=pltpu.CompilerParams(vmem_limit_bytes=38 * MIB),
            name="local_part",
        )(hbm(x), *[hbm(t.reshape(1, D)) for t in (ln_attn_gamma, ln_attn_beta, ln_mlp_gamma, ln_mlp_beta)],
          hbm(wq), hbm(wo), hbm(w_up), hbm(w_down), hbm(k_cache), hbm(v_cache), positions, hbm(pos2))

        n = len(PARTS)
        block = pltpu.VMEM((NR, G, S, H), BF16)
        kblock = pltpu.VMEM((NR - CH, G, S, H), BF16)
        kpblock = pltpu.VMEM((CH, G, S, H), BF16)
        k2, v2, o = pl.pallas_call(
            reduce_kernel,
            out_shape=(kblock, block, pltpu.VMEM((B, D), BF16)),
            in_specs=[anyspace] * 2 + [vm] * 9,
            out_specs=(vm,) * 3,
            scratch_shapes=[
                pltpu.VMEM((G * H, 2 * CH), BF16), pltpu.VMEM((2 * CH, S), BF16),
                pltpu.VMEM((2 * CH, H), F32), pltpu.VMEM((CH, G * H), BF16), pltpu.VMEM((NR, D), BF16), pltpu.VMEM((B // 2, D), BF16),
                pltpu.VMEM((B // 2, D), BF16), pltpu.VMEM((3, B // 2, D // 4), BF16), pltpu.VMEM((B, D), BF16),
                dma((NR // NG - PER,)), dma((NR // NG,)),
                dma((n,)), dma((n,)), dma((n, 3)), dma((n, 3)), dma((n, 3)), dma((n, 3)), dma((n,)), dma((n,)),
            ],
            compiler_params=pltpu.CompilerParams(vmem_limit_bytes=16 * MIB, collective_id=0, has_side_effects=True),
            name="reduce_part",
        )(hbm(k_cache), hbm(v_cache), q, kn, vn, m, part, xv, wov, kp, pos2)

        _, _, _, kf, vf, out = pl.pallas_call(
            write_kernel,
            out_shape=(kpblock, kblock, block, cache, cache, jax.ShapeDtypeStruct((B, D), BF16)),
            in_specs=[vm] * 6 + [sm] + [anyspace] * 2,
            out_specs=(vm,) * 3 + (anyspace,) * 3,
            scratch_shapes=[dma((2 * (NR // NG) + 1,))],
            input_output_aliases={0: 0, 1: 1, 2: 2, 7: 3, 8: 4},
            compiler_params=pltpu.CompilerParams(vmem_limit_bytes=4 * MIB),
            name="write_part",
        )(kp, k2, v2, o, kn, vn, positions, k0, v0)
        return out, kf, vf

    return jax.shard_map(device_step, mesh=mesh, in_specs=(row_spec, vec_spec, vec_spec, vec_spec, vec_spec, P(None, 'tp', None, None), P('tp', None, None, None), P(None, 'tp'), P('tp', None), cache_spec, cache_spec, P('dp')), out_specs=(row_spec, cache_spec, cache_spec), check_vma=False)
```

```python
import functools
import math

import jax
import jax.numpy as jnp
from jax import lax
from jax.experimental import pallas as pl
from jax.experimental.pallas import tpu as pltpu
from jax.sharding import PartitionSpec as P

LN_EPS = 1e-5
ROPE_BASE = 10000.0
NEG_BIG = -1e30
MESH = pl.DeviceIdType.MESH
F32 = jnp.float32
BF16 = jnp.bfloat16

B = 256
D = 2048
S = 128
H = 128
G = 2
FL = 1024
R0 = 64
CH = 64
NG = 16
GI = 2
SCALE = H ** -0.5
PER = CH // NG


def dot(a, b):
    return jnp.dot(a, b, preferred_element_type=F32)


def iota(shape, dim):
    return lax.broadcasted_iota(jnp.int32, shape, dim)


def build_queries(q_ref, row, qt_ref):
    stacked = jnp.concatenate([q_ref[pl.ds(row, CH), pl.ds(0, H)], q_ref[pl.ds(row, CH), pl.ds(H, H)]], axis=0)
    turned = stacked.T
    low = iota((H, 2 * CH), 1) < CH
    qt_ref[pl.ds(0, H), :] = jnp.where(low, turned, 0.0).astype(BF16)
    qt_ref[pl.ds(H, H), :] = jnp.where(low, 0.0, turned).astype(BF16)


def aligned(row):
    return pl.ds(row if isinstance(row, int) else pl.multiple_of(row, NG), NG)


def add_rows(buf, new_ref, pos_s, row, at):
    rows = aligned(row)
    new = [new_ref[rows, pl.ds(g * H, H)] for g in range(G)]
    inside = iota((NG, H), 0).astype(F32).astype(BF16)
    for u in range(NG):
        pos = pos_s[row + u]
        start = pl.multiple_of(lax.shift_left(lax.shift_right_logical(pos, 4), 4), NG)
        mask = inside == jnp.full((NG, H), (pos - start).astype(F32), F32).astype(BF16)
        for g in range(G):
            tile = buf.at[at + u, g, pl.ds(start, NG), :]
            tile[...] = jnp.where(mask, jnp.broadcast_to(new[g][u:u + 1], (NG, H)).astype(BF16), tile[...])


def scores_of_group(kbuf, qt_ref, acc, at, local):
    lane = iota((S, 2 * CH), 1) & (CH - 1)
    for u in range(NG):
        keys = jnp.concatenate([kbuf[at + u, g] for g in range(G)], axis=1)
        acc = jnp.where(lane == local + u, dot(keys, qt_ref[...]), acc)
    return acc


def attend_scores(c, at, wait, also, kbuf, q_ref, kn_ref, pos_v, qt_v, p_v, pn_v, between=None):
    build_queries(q_ref, c * CH, qt_v)
    rows = pl.ds(c * CH, CH)
    with_new = jnp.concatenate([q_ref[rows, pl.ds(g * H, H)] * kn_ref[rows, pl.ds(g * H, H)] for g in range(G)], axis=0)
    s_new = jnp.sum(with_new.T, axis=0, keepdims=True)
    new_at = pos_columns(pos_v, c)

    def step(j, acc):
        for w in range(GI):
            wait(j * GI + w)
        for w in range(GI):
            i = j * GI + w
            acc = scores_of_group(kbuf, qt_v, acc, at + i * NG, i * NG)
            also(i)
        return acc

    acc = jnp.zeros((S, 2 * CH), F32)
    if between is None:
        acc = lax.fori_loop(0, PER // GI, step, acc)
    else:
        for j in range(PER // GI):
            acc = step(j, acc)
            if j == 0:
                between()
    slot = iota((S, 2 * CH), 0)
    s = jnp.where(slot < new_at, acc * SCALE, jnp.where(slot == new_at, s_new * SCALE, NEG_BIG))
    p = softmax_slots(s).astype(BF16).astype(F32)
    p_v[...] = jnp.where(slot == new_at, 0.0, p).T.astype(BF16)
    p_new = jnp.sum(jnp.where(slot == new_at, p, 0.0), axis=0, keepdims=True)
    pn_v[...] = jnp.broadcast_to(p_new, (2 * CH, H)).T


def attend_context(c, at, lo, hi, wait, also, vbuf, vn_ref, p_v, pn_v, ctx_v, between=None):
    def step(j):
        for w in range(GI):
            wait(lo + j * GI + w)
        for w in range(GI):
            i = lo + j * GI + w
            ctx = context_of_group(vbuf, p_v, at + i * NG, i * NG)
            rows = aligned(c * CH + i * NG)
            for g in range(G):
                new = pn_v[aligned(g * CH + i * NG), :] * vn_ref[rows, pl.ds(g * H, H)]
                ctx_v[aligned(i * NG), pl.ds(g * H, H)] = (ctx[g] + new).astype(BF16)
            also(i)

    if between is None:
        pl.loop(0, (hi - lo) // GI)(step)
    else:
        for j in range((hi - lo) // GI):
            step(j)
            if j == 0:
                between()


def pos_columns(pos_v, chunk):
    row = pos_v[pl.ds(chunk // 2, 1), :]
    lane = iota((1, 2 * CH), 1)
    turned = pltpu.roll(row, CH, 1)
    return jnp.where(lane < CH, row, turned) if chunk % 2 == 0 else jnp.where(lane < CH, turned, row)


def softmax_slots(s):
    e = jnp.exp(s - jnp.max(s, axis=0, keepdims=True))
    return e / jnp.sum(e, axis=0, keepdims=True)


def context_of_group(vbuf, p_ref, at, local):
    rows16 = iota((NG, S), 0).astype(F32).astype(BF16)
    zero = jnp.zeros((NG, S), BF16)
    total = []
    for g in range(G):
        probs = p_ref[aligned(g * CH + local), :]
        tot = None
        for u in range(0, NG, 2):
            ps = [jnp.where(rows16 == jnp.asarray(u + w, BF16), probs, zero) for w in range(2)]
            vs = [vbuf[at + u + w, g] for w in range(2)]
            part = dot(jnp.concatenate(ps, axis=1), jnp.concatenate(vs, axis=0))
            tot = part if tot is None else tot + part
        total.append(tot)
    return total


def local_kernel(x_h, ga_h, ba_h, gm_h, bm_h, wq_h, wo_h, wu_h, wd_h, k_h, v_h, pos_s, pos_h,
                 ko_h, vo_h, q_o, kn_o, vn_o, m_o, part_o, x_v, wo_v, kp_o,
                 ln_v, wq_v, w32_v, wqb_v, wu_v, wd_v, kb, vb, pos_v, ain_v, min_v, cos_v, sin_v, h_v, qt_v, p_v, pn_v, ctx_v, a_v,
                 sem_in, sem_k, sem_v, sem_ko, sem_vo, sem_kp):
    ngr = R0 // NG

    def rd(src, dst, i):
        c = pltpu.make_async_copy(src, dst, sem_in.at[i])
        c.start()
        return c

    c_pos = rd(pos_h, pos_v, 0)
    c_x = [rd(x_h.at[pl.ds(64 * i, 64)], x_v.at[pl.ds(64 * i, 64)], 15 + i) for i in range(4)]
    c_ln = [rd(r, ln_v.at[pl.ds(8 * i, 1)], 2 + i) for i, r in enumerate((ga_h, ba_h, gm_h, bm_h))]
    c_wq = [rd(wq_h.at[pl.ds(3072 * i, 3072)], wq_v.at[pl.ds(3072 * i, 3072)], 6 + i) for i in range(4)]

    def kcopy(i, a, b, sem):
        return pltpu.make_async_copy(a.at[pl.ds(NG * i, NG)], b.at[pl.ds(NG * i, NG)], sem.at[i])

    kp_copies = [pltpu.make_async_copy(k_h.at[pl.ds(R0 + NG * i, NG)], kp_o.at[pl.ds(NG * i, NG)], sem_kp.at[i]) for i in range(PER)]

    c_pos.wait()
    lane = iota((S, H), 1)
    inv = jnp.exp((lane & (H // 2 - 1)).astype(F32) * (-2.0 * math.log(ROPE_BASE) / H))
    for i in range(2):
        at = jnp.broadcast_to(pos_v[pl.ds(i, 1), :].astype(F32), (S, H)).T
        ang = at * inv
        sn = jnp.sin(ang)
        cos_v[pl.ds(S * i, S), :] = jnp.cos(ang)
        sin_v[pl.ds(S * i, S), :] = jnp.where(lane < H // 2, -sn, sn)

    for c in c_ln + c_x:
        c.wait()
    for i in range(PER):
        kcopy(i, k_h, kb, sem_k).start()
    RB = 16
    NB = 4

    @pl.loop(0, B // (RB * NB))
    def _(i):
        rows = [pl.ds(pl.multiple_of(i * (RB * NB) + RB * w, RB), RB) for w in range(NB)]

        def tile(r, j):
            return x_v[r, pl.ds(128 * j, 128)].astype(F32)

        means, scales = [], []
        for r in rows:
            tot = tile(r, 0)
            for j in range(1, 16):
                tot = tot + tile(r, j)
            means.append(jnp.sum(tot, axis=-1, keepdims=True) * (1.0 / D))
        for r, mean in zip(rows, means):
            tot = jnp.zeros((RB, 128), F32)
            for j in range(16):
                d = tile(r, j) - mean
                tot = tot + d * d
            scales.append(lax.rsqrt(jnp.sum(tot, axis=-1, keepdims=True) * (1.0 / D) + LN_EPS))
        for r, mean, rs in zip(rows, means, scales):
            for j in range(16):
                cs = pl.ds(128 * j, 128)
                n = (tile(r, j) - mean) * rs
                ain_v[r, cs] = (n * ln_v[pl.ds(0, 1), cs] + ln_v[pl.ds(8, 1), cs]).astype(BF16)
                min_v[r, cs] = (n * ln_v[pl.ds(16, 1), cs] + ln_v[pl.ds(24, 1), cs]).astype(BF16)

    for c in c_wq:
        c.wait()
    for i in range(PER):
        kcopy(i, v_h, vb, sem_v).start()
    c_wo = rd(wo_h, wo_v, 10)
    c_wu = [rd(wu_h.at[pl.ds(1024 * i, 1024)], wu_v.at[pl.ds(1024 * i, 1024)], 11 + i) for i in range(2)]

    @pl.loop(0, 16)
    def _(i):
        w32_v[...] = wq_v[pl.ds(pl.multiple_of(i * 768, 768), 768), :].astype(F32)
        for j in range(3):
            for g in range(G):
                wqb_v[pl.ds(pl.multiple_of(i * 128, 128), 128), pl.ds((g * 3 + j) * H, H)] = (
                    w32_v[pl.ds(2 * j + g, 128, stride=6), :].astype(BF16))

    def rotary(u, r):
        return u * cos_v[r, :] + pltpu.roll(u, H // 2, 1) * sin_v[r, :]

    for n in range(3):
        qkv = dot(ain_v[...], wqb_v[:, pl.ds(256 * n, 256)]).astype(BF16).astype(F32)
        for w in range(2):
            g, j = divmod(2 * n + w, 3)
            u = qkv[:, w * H:(w + 1) * H]
            dst = (q_o, kn_o, vn_o)[j]
            if j < 2:
                u = rotary(u, pl.ds(0, B)).astype(BF16).astype(F32)
            dst[:, pl.ds(g * H, H)] = u

    for c in range(R0 // CH):
        c_wd = [rd(wd_h.at[pl.ds(512 * i, 512)], wd_v.at[pl.ds(512 * i, 512)], 13 + i) for i in range(2)]
        base = c * CH

        def wait_k(i, c=c):
            kcopy(c * PER + i, k_h, kb, sem_k).wait()

        def wait_v(i, c=c):
            kcopy(c * PER + i, v_h, vb, sem_v).wait()

        def old_v(i, c=c):
            if c > 0:
                add_rows(vb, vn_o, pos_s, base - CH + i * NG, base - CH + i * NG)

        def add_k(i):
            add_rows(kb, kn_o, pos_s, base + i * NG, base + i * NG)

        attend_scores(c, base, wait_k, old_v, kb, q_o, kn_o, pos_v, qt_v, p_v, pn_v)
        if c > 0:
            for j in range(PER):
                kcopy((c - 1) * PER + j, vb, vo_h, sem_vo).start()
        for cp in kp_copies:
            cp.start()
        attend_context(c, base, 0, PER, wait_v, add_k, vb, vn_o, p_v, pn_v, ctx_v)
        if c == 0:
            c_wo.wait()
        for n in range(8):
            a_v[pl.ds(base, CH), pl.ds(256 * n, 256)] = dot(ctx_v[...], wo_v[:, pl.ds(256 * n, 256)])
        for j in range(PER):
            kcopy(c * PER + j, kb, ko_h, sem_ko).start()

    for c in c_wu:
        c.wait()
    for n in range(4):
        u = dot(min_v[...], wu_v[:, pl.ds(256 * n, 256)])
        h_v[:, pl.ds(256 * n, 256)] = (0.5 * u * (1.0 + lax.erf(u * (2.0 ** -0.5)))).astype(BF16)
        add_rows(vb, vn_o, pos_s, R0 - CH + n * NG, R0 - CH + n * NG)
    for c in c_wd:
        c.wait()
    for n in range(8):
        cs = pl.ds(256 * n, 256)
        m_o[:, cs] = dot(h_v[...], wd_v[:, cs])
        if n == 0:
            for j in range(PER):
                kcopy(R0 // NG - PER + j, vb, vo_h, sem_vo).start()
        part_o[:, cs] = (a_v[:, cs] + m_o[pl.ds(0, R0), cs]).astype(BF16)

    for cp in kp_copies:
        cp.wait()
    for i in range(ngr):
        kcopy(i, kb, ko_h, sem_ko).wait()
        kcopy(i, vb, vo_h, sem_vo).wait()


PARTS = ((0, 64), (64, 64), (128, 64), (192, 32), (224, 32))


def reduce_kernel(k_h, v_h, q_i, kn_i, vn_i, m_i, part_i, x_v, wo_v, kp_i, pos_i,
                  k2, v2, out_o,
                  qt_v, p_v, pn_v, ctx_v, part_v, d2_v, sum_v, rs_v, gat_v,
                  sem_k, sem_v, s_d, r_d, s_rs, r_rs, s_ag, r_ag, s_e, r_e):
    tp = lax.axis_index("tp")
    core = tp % 2
    chip = tp // 2
    first = R0 // CH
    per = CH // NG
    QC = D // 4

    def kcopy(i):
        return pltpu.make_async_copy(k_h.at[pl.ds(R0 + CH + NG * i, NG)], k2.at[pl.ds(NG * i, NG)], sem_k.at[i])

    def vcopy(i):
        return pltpu.make_async_copy(v_h.at[pl.ds(R0 + NG * i, NG)], v2.at[pl.ds(NG * i, NG)], sem_v.at[i])

    def issue_k(c):
        for i in range(per):
            kcopy((c - first - 1) * per + i).start()

    def issue_v(c):
        for i in range(per):
            vcopy((c - first) * per + i).start()

    issue_v(1)

    sib = tp + 1 - 2 * core
    peers = []
    for k in range(1, 4):
        chip_k = (chip // 2 + k // 2) % 2 * 2 + (chip % 2 + k % 2) % 2
        peers.append((chip_k, chip_k * 2 + core))

    barrier = pltpu.get_barrier_semaphore()
    for t in [sib] + [p for _, p in peers]:
        pl.semaphore_signal(barrier, inc=1, device_id={"tp": t}, device_id_type=MESH)
    my_cols = pl.ds(pl.multiple_of(chip * QC, QC), QC)

    def remote(src, dst, s, r, t):
        return pltpu.make_async_remote_copy(src_ref=src, dst_ref=dst, send_sem=s, recv_sem=r, device_id={"tp": t}, device_id_type=MESH)

    def part_of(c, which):
        start, n = PARTS[c]
        ref, base = (part_i, start) if start < R0 else (part_v, start - R0)
        return ref.at[pl.ds(pl.multiple_of(base + which * (n // 2), NG), n // 2)]

    def half(c):
        start, n = PARTS[c]
        return pl.ds(start // 2, n // 2)

    def out_rows(c):
        start, n = PARTS[c]
        return pl.ds(pl.multiple_of(start + core * (n // 2), NG), n // 2)

    def a_copy(c):
        return remote(part_of(c, 1 - core), d2_v.at[half(c)], s_d.at[c], r_d.at[c], sib)

    def b_copies(c):
        return [remote(sum_v.at[half(c), pl.ds(pl.multiple_of(ck * QC, QC), QC)], rs_v.at[k, half(c)], s_rs.at[c, k], r_rs.at[c, k], t)
                for k, (ck, t) in enumerate(peers)]

    def c_copies(c):
        piece = gat_v.at[out_rows(c), my_cols]
        return [remote(piece, piece, s_ag.at[c, k], r_ag.at[c, k], t) for k, (_, t) in enumerate(peers)]

    def d_copy(c):
        rows = gat_v.at[out_rows(c)]
        return remote(rows, rows, s_e.at[c], r_e.at[c], sib)

    def step_a(c):
        a_copy(c).start()

    def step_b(c):
        a_copy(c).wait_recv()
        sum_v[half(c)] = (part_of(c, core)[...].astype(F32) + d2_v[half(c)].astype(F32)).astype(BF16)
        for cp in b_copies(c):
            cp.start()

    def step_c(c):
        tot = sum_v[half(c), my_cols].astype(F32) + x_v[out_rows(c), my_cols].astype(F32)
        for k, cp in enumerate(b_copies(c)):
            cp.wait_recv()
            tot = tot + rs_v[k, half(c)].astype(F32)
        gat_v[out_rows(c), my_cols] = tot.astype(BF16)
        for cp in c_copies(c):
            cp.start()

    def step_d(c):
        for cp in c_copies(c):
            cp.wait_recv()
        d_copy(c).start()

    def nothing(i):
        pass

    def scores(c, between):
        if c == first:
            attend_scores(c, 0, nothing, nothing, kp_i, q_i, kn_i, pos_i, qt_v, p_v, pn_v, between)
        else:
            at = (c - first - 1) * per
            attend_scores(c, at * NG, lambda i: kcopy(at + i).wait(), nothing, k2, q_i, kn_i, pos_i, qt_v, p_v, pn_v, between)

    def context(c, lo, hi, between):
        at = (c - first) * CH
        attend_context(c, at, lo, hi, lambda i: vcopy((c - first) * per + i).wait(), nothing, v2, vn_i, p_v, pn_v, ctx_v, between)
        n = (hi - lo) * NG
        for k in range(8):
            cs = pl.ds(256 * k, 256)
            part_v[pl.ds(at + lo * NG, n), cs] = (
                dot(ctx_v[pl.ds(lo * NG, n), :], wo_v[:, cs]) + m_i[pl.ds(c * CH + lo * NG, n), cs]).astype(BF16)

    pl.semaphore_wait(barrier, 4)
    step_a(0)
    def between1():
        issue_k(2)

    scores(1, between1)
    step_b(0)
    def between2():
        issue_v(2)

    context(1, 0, per, between2)
    step_a(1)
    def between3():
        issue_k(3)

    scores(2, between3)
    step_b(1)
    def between4():
        issue_v(3)

    context(2, 0, per, between4)
    step_a(2)
    def between5():
        step_b(2)

    scores(3, between5)
    step_c(0)
    def between6():
        pass

    context(3, 0, per // 2, between6)
    step_a(3)
    def between7():
        pass

    context(3, per // 2, per, between7)
    step_a(4)
    step_b(3)
    step_b(4)
    step_c(1)
    step_c(2)
    step_c(3)
    step_c(4)
    step_d(0)
    step_d(1)
    step_d(2)
    step_d(3)
    step_d(4)
    for c in range(len(PARTS)):
        a_copy(c).wait_send()
        for cp in b_copies(c):
            cp.wait_send()
        for cp in c_copies(c):
            cp.wait_send()
        d_copy(c).wait()
    out_o[...] = gat_v[...]


def write_kernel(kp_i, k_i, v_i, o_i, kn_i, vn_i, pos_s, k0_h, v0_h, kp3, k3, v3, ko_h, vo_h, o_h, sem):
    n = (B - R0) // NG
    c_out = pltpu.make_async_copy(o_i, o_h, sem.at[2 * n])
    c_out.start()

    def copy(src, dst, i, k):
        return pltpu.make_async_copy(src.at[pl.ds(NG * i, NG)], dst.at[pl.ds(R0 + NG * k, NG)], sem.at[k if dst is ko_h else n + k])

    late = None
    for src, dst, new, first, count in ((kp3, ko_h, kn_i, 0, PER), (v3, vo_h, vn_i, 0, n), (k3, ko_h, kn_i, PER, n - PER)):
        add_rows(src, new, pos_s, R0 + first * NG, 0)
        if late is not None:
            late.start()

        @pl.loop(1, count)
        def _(i, src=src, dst=dst, new=new, first=first):
            add_rows(src, new, pos_s, R0 + (first + i) * NG, i * NG)
            copy(src, dst, i - 1, first + i - 1).start()

        late = copy(src, dst, count - 1, first + count - 1)
    c_out.wait()
    late.start()

    for src, dst, first, count in ((kp3, ko_h, 0, PER), (v3, vo_h, 0, n), (k3, ko_h, PER, n - PER)):
        @pl.loop(0, count)
        def _(i, src=src, dst=dst, first=first):
            copy(src, dst, i, first + i).wait()


def solution(mesh):
    row_spec = P('dp', None)
    vec_spec = P(None)
    cache_spec = P('dp', 'tp', None, None)
    vm = pl.BlockSpec(memory_space=pltpu.VMEM)
    sm = pl.BlockSpec(memory_space=pltpu.SMEM)
    anyspace = pl.BlockSpec(memory_space=pl.ANY)
    dma = pltpu.SemaphoreType.DMA
    MIB = 1024 * 1024

    def hbm(t):
        return pltpu.with_memory_space_constraint(t, pltpu.HBM)

    def device_step(x, ln_attn_gamma, ln_attn_beta, ln_mlp_gamma, ln_mlp_beta, w_qkv, w_out, w_up, w_down, k_cache, v_cache, positions):
        wq = w_qkv.transpose(0, 2, 1, 3).reshape(D * 3 * G, H)
        wo = w_out.reshape(G * H, D)
        pos2 = positions.reshape(2, 128)
        cache = jax.ShapeDtypeStruct((B, G, S, H), BF16)
        NR = B - R0
        k0, v0, q, kn, vn, m, part, xv, wov, kp = pl.pallas_call(
            local_kernel,
            out_shape=(cache, cache) + (pltpu.VMEM((B, G * H), F32),) * 3 + (pltpu.VMEM((B, D), F32), pltpu.VMEM((R0, D), BF16), pltpu.VMEM((B, D), BF16),
                                                                              pltpu.VMEM((G * H, D), BF16), pltpu.VMEM((CH, G, S, H), BF16)),
            in_specs=[anyspace] * 11 + [sm, anyspace],
            out_specs=(anyspace, anyspace) + (vm,) * 8,
            scratch_shapes=[
                pltpu.VMEM((32, D), F32), pltpu.VMEM((D * 3 * G, H), BF16), pltpu.VMEM((768, H), F32),
                pltpu.VMEM((D, 768), BF16), pltpu.VMEM((D, FL), BF16), pltpu.VMEM((FL, D), BF16),
                pltpu.VMEM((R0, G, S, H), BF16), pltpu.VMEM((R0, G, S, H), BF16), pltpu.VMEM((2, 128), jnp.int32),
                pltpu.VMEM((B, D), BF16), pltpu.VMEM((B, D), BF16), pltpu.VMEM((B, H), F32), pltpu.VMEM((B, H), F32),
                pltpu.VMEM((B, FL), BF16), pltpu.VMEM((G * H, 2 * CH), BF16), pltpu.VMEM((2 * CH, S), BF16), pltpu.VMEM((2 * CH, H), F32),
                pltpu.VMEM((CH, G * H), BF16), pltpu.VMEM((R0, D), F32),
                dma((19,)), dma((R0 // NG,)), dma((R0 // NG,)), dma((R0 // NG,)), dma((R0 // NG,)), dma((PER,)),
            ],
            compiler_params=pltpu.CompilerParams(vmem_limit_bytes=38 * MIB),
            name="local_part",
        )(hbm(x), *[hbm(t.reshape(1, D)) for t in (ln_attn_gamma, ln_attn_beta, ln_mlp_gamma, ln_mlp_beta)],
          hbm(wq), hbm(wo), hbm(w_up), hbm(w_down), hbm(k_cache), hbm(v_cache), positions, hbm(pos2))

        n = len(PARTS)
        block = pltpu.VMEM((NR, G, S, H), BF16)
        kblock = pltpu.VMEM((NR - CH, G, S, H), BF16)
        kpblock = pltpu.VMEM((CH, G, S, H), BF16)
        k2, v2, o = pl.pallas_call(
            reduce_kernel,
            out_shape=(kblock, block, pltpu.VMEM((B, D), BF16)),
            in_specs=[anyspace] * 2 + [vm] * 9,
            out_specs=(vm,) * 3,
            scratch_shapes=[
                pltpu.VMEM((G * H, 2 * CH), BF16), pltpu.VMEM((2 * CH, S), BF16),
                pltpu.VMEM((2 * CH, H), F32), pltpu.VMEM((CH, G * H), BF16), pltpu.VMEM((NR, D), BF16), pltpu.VMEM((B // 2, D), BF16),
                pltpu.VMEM((B // 2, D), BF16), pltpu.VMEM((3, B // 2, D // 4), BF16), pltpu.VMEM((B, D), BF16),
                dma((NR // NG - PER,)), dma((NR // NG,)),
                dma((n,)), dma((n,)), dma((n, 3)), dma((n, 3)), dma((n, 3)), dma((n, 3)), dma((n,)), dma((n,)),
            ],
            compiler_params=pltpu.CompilerParams(vmem_limit_bytes=16 * MIB, collective_id=0, has_side_effects=True),
            name="reduce_part",
        )(hbm(k_cache), hbm(v_cache), q, kn, vn, m, part, xv, wov, kp, pos2)

        _, _, _, kf, vf, out = pl.pallas_call(
            write_kernel,
            out_shape=(kpblock, kblock, block, cache, cache, jax.ShapeDtypeStruct((B, D), BF16)),
            in_specs=[vm] * 6 + [sm] + [anyspace] * 2,
            out_specs=(vm,) * 3 + (anyspace,) * 3,
            scratch_shapes=[dma((2 * (NR // NG) + 1,))],
            input_output_aliases={0: 0, 1: 1, 2: 2, 7: 3, 8: 4},
            compiler_params=pltpu.CompilerParams(vmem_limit_bytes=4 * MIB),
            name="write_part",
        )(kp, k2, v2, o, kn, vn, positions, k0, v0)
        return out, kf, vf

    return jax.shard_map(device_step, mesh=mesh, in_specs=(row_spec, vec_spec, vec_spec, vec_spec, vec_spec, P(None, 'tp', None, None), P('tp', None, None, None), P(None, 'tp'), P('tp', None), cache_spec, cache_spec, P('dp')), out_specs=(row_spec, cache_spec, cache_spec), check_vma=False)
```

```python
import functools
import math

import jax
import jax.numpy as jnp
from jax import lax
from jax.experimental import pallas as pl
from jax.experimental.pallas import tpu as pltpu
from jax.sharding import PartitionSpec as P

LN_EPS = 1e-5
ROPE_BASE = 10000.0
NEG_BIG = -1e30
MESH = pl.DeviceIdType.MESH
F32 = jnp.float32
BF16 = jnp.bfloat16

B = 256
D = 2048
S = 128
H = 128
G = 2
FL = 1024
R0 = 64
CH = 64
NG = 16
GI = 2
SCALE = H ** -0.5
PER = CH // NG


def dot(a, b):
    return jnp.dot(a, b, preferred_element_type=F32)


def iota(shape, dim):
    return lax.broadcasted_iota(jnp.int32, shape, dim)


def build_queries(q_ref, row, qt_ref):
    stacked = jnp.concatenate([q_ref[pl.ds(row, CH), pl.ds(0, H)], q_ref[pl.ds(row, CH), pl.ds(H, H)]], axis=0)
    turned = stacked.T
    low = iota((H, 2 * CH), 1) < CH
    qt_ref[pl.ds(0, H), :] = jnp.where(low, turned, 0.0).astype(BF16)
    qt_ref[pl.ds(H, H), :] = jnp.where(low, 0.0, turned).astype(BF16)


def aligned(row):
    return pl.ds(row if isinstance(row, int) else pl.multiple_of(row, NG), NG)


def add_rows(buf, new_ref, pos_s, row, at):
    rows = aligned(row)
    new = [new_ref[rows, pl.ds(g * H, H)] for g in range(G)]
    inside = iota((NG, H), 0).astype(F32).astype(BF16)
    for u in range(NG):
        pos = pos_s[row + u]
        start = pl.multiple_of(lax.shift_left(lax.shift_right_logical(pos, 4), 4), NG)
        mask = inside == jnp.full((NG, H), (pos - start).astype(F32), F32).astype(BF16)
        for g in range(G):
            tile = buf.at[at + u, g, pl.ds(start, NG), :]
            tile[...] = jnp.where(mask, jnp.broadcast_to(new[g][u:u + 1], (NG, H)).astype(BF16), tile[...])


def scores_of_group(kbuf, qt_ref, acc, at, local):
    lane = iota((S, 2 * CH), 1) & (CH - 1)
    for u in range(NG):
        keys = jnp.concatenate([kbuf[at + u, g] for g in range(G)], axis=1)
        acc = jnp.where(lane == local + u, dot(keys, qt_ref[...]), acc)
    return acc


def attend_scores(c, at, wait, also, kbuf, q_ref, kn_ref, pos_v, qt_v, p_v, pn_v, between=None):
    build_queries(q_ref, c * CH, qt_v)
    rows = pl.ds(c * CH, CH)
    with_new = jnp.concatenate([q_ref[rows, pl.ds(g * H, H)] * kn_ref[rows, pl.ds(g * H, H)] for g in range(G)], axis=0)
    s_new = jnp.sum(with_new.T, axis=0, keepdims=True)
    new_at = pos_columns(pos_v, c)

    def step(j, acc):
        for w in range(GI):
            wait(j * GI + w)
        for w in range(GI):
            i = j * GI + w
            acc = scores_of_group(kbuf, qt_v, acc, at + i * NG, i * NG)
            also(i)
        return acc

    acc = jnp.zeros((S, 2 * CH), F32)
    if between is None:
        acc = lax.fori_loop(0, PER // GI, step, acc)
    else:
        for j in range(PER // GI):
            acc = step(j, acc)
            if j == 0:
                between()
    slot = iota((S, 2 * CH), 0)
    s = jnp.where(slot < new_at, acc * SCALE, jnp.where(slot == new_at, s_new * SCALE, NEG_BIG))
    p = softmax_slots(s).astype(BF16).astype(F32)
    p_v[...] = jnp.where(slot == new_at, 0.0, p).T.astype(BF16)
    p_new = jnp.sum(jnp.where(slot == new_at, p, 0.0), axis=0, keepdims=True)
    pn_v[...] = jnp.broadcast_to(p_new, (2 * CH, H)).T


def attend_context(c, at, lo, hi, wait, also, vbuf, vn_ref, p_v, pn_v, ctx_v, between=None):
    def step(j):
        for w in range(GI):
            wait(lo + j * GI + w)
        for w in range(GI):
            i = lo + j * GI + w
            ctx = context_of_group(vbuf, p_v, at + i * NG, i * NG)
            rows = aligned(c * CH + i * NG)
            for g in range(G):
                new = pn_v[aligned(g * CH + i * NG), :] * vn_ref[rows, pl.ds(g * H, H)]
                ctx_v[aligned(i * NG), pl.ds(g * H, H)] = (ctx[g] + new).astype(BF16)
            also(i)

    if between is None:
        pl.loop(0, (hi - lo) // GI)(step)
    else:
        for j in range((hi - lo) // GI):
            step(j)
            if j == 0:
                between()


def pos_columns(pos_v, chunk):
    row = pos_v[pl.ds(chunk // 2, 1), :]
    lane = iota((1, 2 * CH), 1)
    turned = pltpu.roll(row, CH, 1)
    return jnp.where(lane < CH, row, turned) if chunk % 2 == 0 else jnp.where(lane < CH, turned, row)


def softmax_slots(s):
    e = jnp.exp(s - jnp.max(s, axis=0, keepdims=True))
    return e / jnp.sum(e, axis=0, keepdims=True)


def context_of_group(vbuf, p_ref, at, local):
    rows16 = iota((NG, S), 0).astype(F32).astype(BF16)
    zero = jnp.zeros((NG, S), BF16)
    total = []
    for g in range(G):
        probs = p_ref[aligned(g * CH + local), :]
        tot = None
        for u in range(0, NG, 2):
            ps = [jnp.where(rows16 == jnp.asarray(u + w, BF16), probs, zero) for w in range(2)]
            vs = [vbuf[at + u + w, g] for w in range(2)]
            part = dot(jnp.concatenate(ps, axis=1), jnp.concatenate(vs, axis=0))
            tot = part if tot is None else tot + part
        total.append(tot)
    return total


def local_kernel(x_h, ga_h, ba_h, gm_h, bm_h, wq_h, wo_h, wu_h, wd_h, k_h, v_h, pos_s, pos_h,
                 ko_h, vo_h, q_o, kn_o, vn_o, m_o, part_o, x_v, wo_v, kp_o,
                 ln_v, wq_v, w32_v, wqb_v, wu_v, wd_v, kb, vb, pos_v, ain_v, min_v, cos_v, sin_v, h_v, qt_v, p_v, pn_v, ctx_v, a_v,
                 sem_in, sem_k, sem_v, sem_ko, sem_vo, sem_kp):
    ngr = R0 // NG

    def rd(src, dst, i):
        c = pltpu.make_async_copy(src, dst, sem_in.at[i])
        c.start()
        return c

    c_pos = rd(pos_h, pos_v, 0)
    c_x = [rd(x_h.at[pl.ds(64 * i, 64)], x_v.at[pl.ds(64 * i, 64)], 15 + i) for i in range(4)]
    c_ln = [rd(r, ln_v.at[pl.ds(8 * i, 1)], 2 + i) for i, r in enumerate((ga_h, ba_h, gm_h, bm_h))]
    c_wq = [rd(wq_h.at[pl.ds(3072 * i, 3072)], wq_v.at[pl.ds(3072 * i, 3072)], 6 + i) for i in range(4)]

    def kcopy(i, a, b, sem):
        return pltpu.make_async_copy(a.at[pl.ds(NG * i, NG)], b.at[pl.ds(NG * i, NG)], sem.at[i])

    kp_copies = [pltpu.make_async_copy(k_h.at[pl.ds(R0 + NG * i, NG)], kp_o.at[pl.ds(NG * i, NG)], sem_kp.at[i]) for i in range(PER)]

    c_pos.wait()
    lane = iota((S, H), 1)
    inv = jnp.exp((lane & (H // 2 - 1)).astype(F32) * (-2.0 * math.log(ROPE_BASE) / H))
    for i in range(2):
        at = jnp.broadcast_to(pos_v[pl.ds(i, 1), :].astype(F32), (S, H)).T
        ang = at * inv
        sn = jnp.sin(ang)
        cos_v[pl.ds(S * i, S), :] = jnp.cos(ang)
        sin_v[pl.ds(S * i, S), :] = jnp.where(lane < H // 2, -sn, sn)

    for c in c_ln + c_x:
        c.wait()
    for i in range(PER):
        kcopy(i, k_h, kb, sem_k).start()
    RB = 16
    NB = 4

    @pl.loop(0, B // (RB * NB))
    def _(i):
        rows = [pl.ds(pl.multiple_of(i * (RB * NB) + RB * w, RB), RB) for w in range(NB)]

        def tile(r, j):
            return x_v[r, pl.ds(128 * j, 128)].astype(F32)

        means, scales = [], []
        for r in rows:
            tot = tile(r, 0)
            for j in range(1, 16):
                tot = tot + tile(r, j)
            means.append(jnp.sum(tot, axis=-1, keepdims=True) * (1.0 / D))
        for r, mean in zip(rows, means):
            tot = jnp.zeros((RB, 128), F32)
            for j in range(16):
                d = tile(r, j) - mean
                tot = tot + d * d
            scales.append(lax.rsqrt(jnp.sum(tot, axis=-1, keepdims=True) * (1.0 / D) + LN_EPS))
        for r, mean, rs in zip(rows, means, scales):
            for j in range(16):
                cs = pl.ds(128 * j, 128)
                n = (tile(r, j) - mean) * rs
                ain_v[r, cs] = (n * ln_v[pl.ds(0, 1), cs] + ln_v[pl.ds(8, 1), cs]).astype(BF16)
                min_v[r, cs] = (n * ln_v[pl.ds(16, 1), cs] + ln_v[pl.ds(24, 1), cs]).astype(BF16)

    for c in c_wq:
        c.wait()
    for i in range(PER):
        kcopy(i, v_h, vb, sem_v).start()
    c_wo = rd(wo_h, wo_v, 10)
    c_wu = [rd(wu_h.at[pl.ds(1024 * i, 1024)], wu_v.at[pl.ds(1024 * i, 1024)], 11 + i) for i in range(2)]

    @pl.loop(0, 16)
    def _(i):
        w32_v[...] = wq_v[pl.ds(pl.multiple_of(i * 768, 768), 768), :].astype(F32)
        for j in range(3):
            for g in range(G):
                wqb_v[pl.ds(pl.multiple_of(i * 128, 128), 128), pl.ds((g * 3 + j) * H, H)] = (
                    w32_v[pl.ds(2 * j + g, 128, stride=6), :].astype(BF16))

    def rotary(u, r):
        return u * cos_v[r, :] + pltpu.roll(u, H // 2, 1) * sin_v[r, :]

    for n in range(3):
        qkv = dot(ain_v[...], wqb_v[:, pl.ds(256 * n, 256)]).astype(BF16).astype(F32)
        for w in range(2):
            g, j = divmod(2 * n + w, 3)
            u = qkv[:, w * H:(w + 1) * H]
            dst = (q_o, kn_o, vn_o)[j]
            if j < 2:
                u = rotary(u, pl.ds(0, B)).astype(BF16).astype(F32)
            dst[:, pl.ds(g * H, H)] = u

    for c in range(R0 // CH):
        c_wd = [rd(wd_h.at[pl.ds(512 * i, 512)], wd_v.at[pl.ds(512 * i, 512)], 13 + i) for i in range(2)]
        base = c * CH

        def wait_k(i, c=c):
            kcopy(c * PER + i, k_h, kb, sem_k).wait()

        def wait_v(i, c=c):
            kcopy(c * PER + i, v_h, vb, sem_v).wait()

        def old_v(i, c=c):
            if c > 0:
                add_rows(vb, vn_o, pos_s, base - CH + i * NG, base - CH + i * NG)

        def add_k(i):
            add_rows(kb, kn_o, pos_s, base + i * NG, base + i * NG)

        attend_scores(c, base, wait_k, old_v, kb, q_o, kn_o, pos_v, qt_v, p_v, pn_v)
        if c > 0:
            for j in range(PER):
                kcopy((c - 1) * PER + j, vb, vo_h, sem_vo).start()
        for cp in kp_copies:
            cp.start()
        attend_context(c, base, 0, PER, wait_v, add_k, vb, vn_o, p_v, pn_v, ctx_v)
        if c == 0:
            c_wo.wait()
        for n in range(8):
            a_v[pl.ds(base, CH), pl.ds(256 * n, 256)] = dot(ctx_v[...], wo_v[:, pl.ds(256 * n, 256)])
        for j in range(PER):
            kcopy(c * PER + j, kb, ko_h, sem_ko).start()

    for c in c_wu:
        c.wait()
    for n in range(4):
        u = dot(min_v[...], wu_v[:, pl.ds(256 * n, 256)])
        h_v[:, pl.ds(256 * n, 256)] = (0.5 * u * (1.0 + lax.erf(u * (2.0 ** -0.5)))).astype(BF16)
        for i in ((0, 1), (2,), (3,), ())[n]:
            add_rows(vb, vn_o, pos_s, R0 - CH + i * NG, R0 - CH + i * NG)
    for j in range(PER):
        kcopy(R0 // NG - PER + j, vb, vo_h, sem_vo).start()
    for c in c_wd:
        c.wait()
    for n in range(8):
        cs = pl.ds(256 * n, 256)
        m_o[:, cs] = dot(h_v[...], wd_v[:, cs])
        part_o[:, cs] = (a_v[:, cs] + m_o[pl.ds(0, R0), cs]).astype(BF16)

    for cp in kp_copies:
        cp.wait()
    for i in range(ngr):
        kcopy(i, kb, ko_h, sem_ko).wait()
        kcopy(i, vb, vo_h, sem_vo).wait()


PARTS = ((0, 64), (64, 64), (128, 64), (192, 32), (224, 32))


def reduce_kernel(k_h, v_h, q_i, kn_i, vn_i, m_i, part_i, x_v, wo_v, kp_i, pos_i,
                  k2, v2, out_o,
                  qt_v, p_v, pn_v, ctx_v, part_v, d2_v, sum_v, rs_v, gat_v,
                  sem_k, sem_v, s_d, r_d, s_rs, r_rs, s_ag, r_ag, s_e, r_e):
    tp = lax.axis_index("tp")
    core = tp % 2
    chip = tp // 2
    first = R0 // CH
    per = CH // NG
    QC = D // 4

    def kcopy(i):
        return pltpu.make_async_copy(k_h.at[pl.ds(R0 + CH + NG * i, NG)], k2.at[pl.ds(NG * i, NG)], sem_k.at[i])

    def vcopy(i):
        return pltpu.make_async_copy(v_h.at[pl.ds(R0 + NG * i, NG)], v2.at[pl.ds(NG * i, NG)], sem_v.at[i])

    def issue_k(c):
        for i in range(per):
            kcopy((c - first - 1) * per + i).start()

    def issue_v(c):
        for i in range(per):
            vcopy((c - first) * per + i).start()

    issue_v(1)

    sib = tp + 1 - 2 * core
    peers = []
    for k in range(1, 4):
        chip_k = (chip // 2 + k // 2) % 2 * 2 + (chip % 2 + k % 2) % 2
        peers.append((chip_k, chip_k * 2 + core))

    barrier = pltpu.get_barrier_semaphore()
    for t in [sib] + [p for _, p in peers]:
        pl.semaphore_signal(barrier, inc=1, device_id={"tp": t}, device_id_type=MESH)
    my_cols = pl.ds(pl.multiple_of(chip * QC, QC), QC)

    def remote(src, dst, s, r, t):
        return pltpu.make_async_remote_copy(src_ref=src, dst_ref=dst, send_sem=s, recv_sem=r, device_id={"tp": t}, device_id_type=MESH)

    def part_of(c, which):
        start, n = PARTS[c]
        ref, base = (part_i, start) if start < R0 else (part_v, start - R0)
        return ref.at[pl.ds(pl.multiple_of(base + which * (n // 2), NG), n // 2)]

    def half(c):
        start, n = PARTS[c]
        return pl.ds(start // 2, n // 2)

    def out_rows(c):
        start, n = PARTS[c]
        return pl.ds(pl.multiple_of(start + core * (n // 2), NG), n // 2)

    def a_copy(c):
        return remote(part_of(c, 1 - core), d2_v.at[half(c)], s_d.at[c], r_d.at[c], sib)

    def b_copies(c):
        return [remote(sum_v.at[half(c), pl.ds(pl.multiple_of(ck * QC, QC), QC)], rs_v.at[k, half(c)], s_rs.at[c, k], r_rs.at[c, k], t)
                for k, (ck, t) in enumerate(peers)]

    def c_copies(c):
        piece = gat_v.at[out_rows(c), my_cols]
        return [remote(piece, piece, s_ag.at[c, k], r_ag.at[c, k], t) for k, (_, t) in enumerate(peers)]

    def d_copy(c):
        rows = gat_v.at[out_rows(c)]
        return remote(rows, rows, s_e.at[c], r_e.at[c], sib)

    def step_a(c):
        a_copy(c).start()

    def step_b(c):
        a_copy(c).wait_recv()
        sum_v[half(c)] = (part_of(c, core)[...].astype(F32) + d2_v[half(c)].astype(F32)).astype(BF16)
        for cp in b_copies(c):
            cp.start()

    def step_c(c):
        tot = sum_v[half(c), my_cols].astype(F32) + x_v[out_rows(c), my_cols].astype(F32)
        for k, cp in enumerate(b_copies(c)):
            cp.wait_recv()
            tot = tot + rs_v[k, half(c)].astype(F32)
        gat_v[out_rows(c), my_cols] = tot.astype(BF16)
        for cp in c_copies(c):
            cp.start()

    def step_d(c):
        for cp in c_copies(c):
            cp.wait_recv()
        d_copy(c).start()

    def nothing(i):
        pass

    def scores(c, between):
        if c == first:
            attend_scores(c, 0, nothing, nothing, kp_i, q_i, kn_i, pos_i, qt_v, p_v, pn_v, between)
        else:
            at = (c - first - 1) * per
            attend_scores(c, at * NG, lambda i: kcopy(at + i).wait(), nothing, k2, q_i, kn_i, pos_i, qt_v, p_v, pn_v, between)

    def context(c, lo, hi, between):
        at = (c - first) * CH
        attend_context(c, at, lo, hi, lambda i: vcopy((c - first) * per + i).wait(), nothing, v2, vn_i, p_v, pn_v, ctx_v, between)
        n = (hi - lo) * NG
        for k in range(8):
            cs = pl.ds(256 * k, 256)
            part_v[pl.ds(at + lo * NG, n), cs] = (
                dot(ctx_v[pl.ds(lo * NG, n), :], wo_v[:, cs]) + m_i[pl.ds(c * CH + lo * NG, n), cs]).astype(BF16)

    pl.semaphore_wait(barrier, 4)
    step_a(0)
    def between1():
        issue_k(2)

    scores(1, between1)
    step_b(0)
    def between2():
        issue_v(2)

    context(1, 0, per, between2)
    step_a(1)
    def between3():
        issue_k(3)

    scores(2, between3)
    step_b(1)
    def between4():
        issue_v(3)

    context(2, 0, per, between4)
    step_a(2)
    def between5():
        step_b(2)

    scores(3, between5)
    step_c(0)
    def between6():
        pass

    context(3, 0, per // 2, between6)
    step_a(3)
    def between7():
        pass

    context(3, per // 2, per, between7)
    step_a(4)
    step_b(3)
    step_b(4)
    step_c(1)
    step_c(2)
    step_c(3)
    step_c(4)
    step_d(0)
    step_d(1)
    step_d(2)
    step_d(3)
    step_d(4)
    for c in range(len(PARTS)):
        a_copy(c).wait_send()
        for cp in b_copies(c):
            cp.wait_send()
        for cp in c_copies(c):
            cp.wait_send()
        d_copy(c).wait()
    out_o[...] = gat_v[...]


def write_kernel(kp_i, k_i, v_i, o_i, kn_i, vn_i, pos_s, k0_h, v0_h, kp3, k3, v3, ko_h, vo_h, o_h, sem):
    n = (B - R0) // NG
    c_out = pltpu.make_async_copy(o_i, o_h, sem.at[2 * n])
    c_out.start()

    def copy(src, dst, i, k):
        return pltpu.make_async_copy(src.at[pl.ds(NG * i, NG)], dst.at[pl.ds(R0 + NG * k, NG)], sem.at[k if dst is ko_h else n + k])

    late = None
    for src, dst, new, first, count in ((kp3, ko_h, kn_i, 0, PER), (v3, vo_h, vn_i, 0, n), (k3, ko_h, kn_i, PER, n - PER)):
        add_rows(src, new, pos_s, R0 + first * NG, 0)
        if late is not None:
            late.start()

        @pl.loop(1, count)
        def _(i, src=src, dst=dst, new=new, first=first):
            add_rows(src, new, pos_s, R0 + (first + i) * NG, i * NG)
            copy(src, dst, i - 1, first + i - 1).start()

        late = copy(src, dst, count - 1, first + count - 1)
    late.start()

    for src, dst, first, count in ((kp3, ko_h, 0, PER), (v3, vo_h, 0, n), (k3, ko_h, PER, n - PER)):
        @pl.loop(0, count)
        def _(i, src=src, dst=dst, first=first):
            copy(src, dst, i, first + i).wait()

    c_out.wait()


def solution(mesh):
    row_spec = P('dp', None)
    vec_spec = P(None)
    cache_spec = P('dp', 'tp', None, None)
    vm = pl.BlockSpec(memory_space=pltpu.VMEM)
    sm = pl.BlockSpec(memory_space=pltpu.SMEM)
    anyspace = pl.BlockSpec(memory_space=pl.ANY)
    dma = pltpu.SemaphoreType.DMA
    MIB = 1024 * 1024

    def hbm(t):
        return pltpu.with_memory_space_constraint(t, pltpu.HBM)

    def device_step(x, ln_attn_gamma, ln_attn_beta, ln_mlp_gamma, ln_mlp_beta, w_qkv, w_out, w_up, w_down, k_cache, v_cache, positions):
        wq = w_qkv.transpose(0, 2, 1, 3).reshape(D * 3 * G, H)
        wo = w_out.reshape(G * H, D)
        pos2 = positions.reshape(2, 128)
        cache = jax.ShapeDtypeStruct((B, G, S, H), BF16)
        NR = B - R0
        k0, v0, q, kn, vn, m, part, xv, wov, kp = pl.pallas_call(
            local_kernel,
            out_shape=(cache, cache) + (pltpu.VMEM((B, G * H), F32),) * 3 + (pltpu.VMEM((B, D), F32), pltpu.VMEM((R0, D), BF16), pltpu.VMEM((B, D), BF16),
                                                                              pltpu.VMEM((G * H, D), BF16), pltpu.VMEM((CH, G, S, H), BF16)),
            in_specs=[anyspace] * 11 + [sm, anyspace],
            out_specs=(anyspace, anyspace) + (vm,) * 8,
            scratch_shapes=[
                pltpu.VMEM((32, D), F32), pltpu.VMEM((D * 3 * G, H), BF16), pltpu.VMEM((768, H), F32),
                pltpu.VMEM((D, 768), BF16), pltpu.VMEM((D, FL), BF16), pltpu.VMEM((FL, D), BF16),
                pltpu.VMEM((R0, G, S, H), BF16), pltpu.VMEM((R0, G, S, H), BF16), pltpu.VMEM((2, 128), jnp.int32),
                pltpu.VMEM((B, D), BF16), pltpu.VMEM((B, D), BF16), pltpu.VMEM((B, H), F32), pltpu.VMEM((B, H), F32),
                pltpu.VMEM((B, FL), BF16), pltpu.VMEM((G * H, 2 * CH), BF16), pltpu.VMEM((2 * CH, S), BF16), pltpu.VMEM((2 * CH, H), F32),
                pltpu.VMEM((CH, G * H), BF16), pltpu.VMEM((R0, D), F32),
                dma((19,)), dma((R0 // NG,)), dma((R0 // NG,)), dma((R0 // NG,)), dma((R0 // NG,)), dma((PER,)),
            ],
            compiler_params=pltpu.CompilerParams(vmem_limit_bytes=38 * MIB),
            name="local_part",
        )(hbm(x), *[hbm(t.reshape(1, D)) for t in (ln_attn_gamma, ln_attn_beta, ln_mlp_gamma, ln_mlp_beta)],
          hbm(wq), hbm(wo), hbm(w_up), hbm(w_down), hbm(k_cache), hbm(v_cache), positions, hbm(pos2))

        n = len(PARTS)
        block = pltpu.VMEM((NR, G, S, H), BF16)
        kblock = pltpu.VMEM((NR - CH, G, S, H), BF16)
        kpblock = pltpu.VMEM((CH, G, S, H), BF16)
        k2, v2, o = pl.pallas_call(
            reduce_kernel,
            out_shape=(kblock, block, pltpu.VMEM((B, D), BF16)),
            in_specs=[anyspace] * 2 + [vm] * 9,
            out_specs=(vm,) * 3,
            scratch_shapes=[
                pltpu.VMEM((G * H, 2 * CH), BF16), pltpu.VMEM((2 * CH, S), BF16),
                pltpu.VMEM((2 * CH, H), F32), pltpu.VMEM((CH, G * H), BF16), pltpu.VMEM((NR, D), BF16), pltpu.VMEM((B // 2, D), BF16),
                pltpu.VMEM((B // 2, D), BF16), pltpu.VMEM((3, B // 2, D // 4), BF16), pltpu.VMEM((B, D), BF16),
                dma((NR // NG - PER,)), dma((NR // NG,)),
                dma((n,)), dma((n,)), dma((n, 3)), dma((n, 3)), dma((n, 3)), dma((n, 3)), dma((n,)), dma((n,)),
            ],
            compiler_params=pltpu.CompilerParams(vmem_limit_bytes=16 * MIB, collective_id=0, has_side_effects=True),
            name="reduce_part",
        )(hbm(k_cache), hbm(v_cache), q, kn, vn, m, part, xv, wov, kp, pos2)

        _, _, _, kf, vf, out = pl.pallas_call(
            write_kernel,
            out_shape=(kpblock, kblock, block, cache, cache, jax.ShapeDtypeStruct((B, D), BF16)),
            in_specs=[vm] * 6 + [sm] + [anyspace] * 2,
            out_specs=(vm,) * 3 + (anyspace,) * 3,
            scratch_shapes=[dma((2 * (NR // NG) + 1,))],
            input_output_aliases={0: 0, 1: 1, 2: 2, 7: 3, 8: 4},
            compiler_params=pltpu.CompilerParams(vmem_limit_bytes=4 * MIB),
            name="write_part",
        )(kp, k2, v2, o, kn, vn, positions, k0, v0)
        return out, kf, vf

    return jax.shard_map(device_step, mesh=mesh, in_specs=(row_spec, vec_spec, vec_spec, vec_spec, vec_spec, P(None, 'tp', None, None), P('tp', None, None, None), P(None, 'tp'), P('tp', None), cache_spec, cache_spec, P('dp')), out_specs=(row_spec, cache_spec, cache_spec), check_vma=False)
```

```python
import functools
import math

import jax
import jax.numpy as jnp
from jax import lax
from jax.experimental import pallas as pl
from jax.experimental.pallas import tpu as pltpu
from jax.sharding import PartitionSpec as P

LN_EPS = 1e-5
ROPE_BASE = 10000.0
NEG_BIG = -1e30
MESH = pl.DeviceIdType.MESH
F32 = jnp.float32
BF16 = jnp.bfloat16

B = 256
D = 2048
S = 128
H = 128
G = 2
FL = 1024
R0 = 64
CH = 64
NG = 16
GI = 2
SCALE = H ** -0.5
PER = CH // NG


def dot(a, b):
    return jnp.dot(a, b, preferred_element_type=F32)


def iota(shape, dim):
    return lax.broadcasted_iota(jnp.int32, shape, dim)


def build_queries(q_ref, row, qt_ref):
    stacked = jnp.concatenate([q_ref[pl.ds(row, CH), pl.ds(0, H)], q_ref[pl.ds(row, CH), pl.ds(H, H)]], axis=0)
    turned = stacked.T
    low = iota((H, 2 * CH), 1) < CH
    qt_ref[pl.ds(0, H), :] = jnp.where(low, turned, 0.0).astype(BF16)
    qt_ref[pl.ds(H, H), :] = jnp.where(low, 0.0, turned).astype(BF16)


def aligned(row):
    return pl.ds(row if isinstance(row, int) else pl.multiple_of(row, NG), NG)


def add_rows(buf, new_ref, pos_s, row, at):
    rows = aligned(row)
    new = [new_ref[rows, pl.ds(g * H, H)] for g in range(G)]
    inside = iota((NG, H), 0).astype(F32).astype(BF16)
    for u in range(NG):
        pos = pos_s[row + u]
        start = pl.multiple_of(lax.shift_left(lax.shift_right_logical(pos, 4), 4), NG)
        mask = inside == jnp.full((NG, H), (pos - start).astype(F32), F32).astype(BF16)
        for g in range(G):
            tile = buf.at[at + u, g, pl.ds(start, NG), :]
            tile[...] = jnp.where(mask, jnp.broadcast_to(new[g][u:u + 1], (NG, H)).astype(BF16), tile[...])


def scores_of_group(kbuf, qt_ref, acc, at, local):
    lane = iota((S, 2 * CH), 1) & (CH - 1)
    for u in range(NG):
        keys = jnp.concatenate([kbuf[at + u, g] for g in range(G)], axis=1)
        acc = jnp.where(lane == local + u, dot(keys, qt_ref[...]), acc)
    return acc


def attend_scores(c, at, wait, also, kbuf, q_ref, kn_ref, pos_v, qt_v, p_v, pn_v, between=None):
    build_queries(q_ref, c * CH, qt_v)
    rows = pl.ds(c * CH, CH)
    with_new = jnp.concatenate([q_ref[rows, pl.ds(g * H, H)] * kn_ref[rows, pl.ds(g * H, H)] for g in range(G)], axis=0)
    s_new = jnp.sum(with_new.T, axis=0, keepdims=True)
    new_at = pos_columns(pos_v, c)

    def step(j, acc):
        for w in range(GI):
            wait(j * GI + w)
        for w in range(GI):
            i = j * GI + w
            acc = scores_of_group(kbuf, qt_v, acc, at + i * NG, i * NG)
            also(i)
        return acc

    acc = jnp.zeros((S, 2 * CH), F32)
    if between is None:
        acc = lax.fori_loop(0, PER // GI, step, acc)
    else:
        for j in range(PER // GI):
            acc = step(j, acc)
            if j == 0:
                between()
    slot = iota((S, 2 * CH), 0)
    s = jnp.where(slot < new_at, acc * SCALE, jnp.where(slot == new_at, s_new * SCALE, NEG_BIG))
    p = softmax_slots(s).astype(BF16).astype(F32)
    p_v[...] = jnp.where(slot == new_at, 0.0, p).T.astype(BF16)
    p_new = jnp.sum(jnp.where(slot == new_at, p, 0.0), axis=0, keepdims=True)
    pn_v[...] = jnp.broadcast_to(p_new, (2 * CH, H)).T


def attend_context(c, at, lo, hi, wait, also, vbuf, vn_ref, p_v, pn_v, ctx_v, between=None):
    def step(j):
        for w in range(GI):
            wait(lo + j * GI + w)
        for w in range(GI):
            i = lo + j * GI + w
            ctx = context_of_group(vbuf, p_v, at + i * NG, i * NG)
            rows = aligned(c * CH + i * NG)
            for g in range(G):
                new = pn_v[aligned(g * CH + i * NG), :] * vn_ref[rows, pl.ds(g * H, H)]
                ctx_v[aligned(i * NG), pl.ds(g * H, H)] = (ctx[g] + new).astype(BF16)
            also(i)

    if between is None:
        pl.loop(0, (hi - lo) // GI)(step)
    else:
        for j in range((hi - lo) // GI):
            step(j)
            if j == 0:
                between()


def pos_columns(pos_v, chunk):
    row = pos_v[pl.ds(chunk // 2, 1), :]
    lane = iota((1, 2 * CH), 1)
    turned = pltpu.roll(row, CH, 1)
    return jnp.where(lane < CH, row, turned) if chunk % 2 == 0 else jnp.where(lane < CH, turned, row)


def softmax_slots(s):
    e = jnp.exp(s - jnp.max(s, axis=0, keepdims=True))
    return e / jnp.sum(e, axis=0, keepdims=True)


def context_of_group(vbuf, p_ref, at, local):
    rows16 = iota((NG, S), 0).astype(F32).astype(BF16)
    zero = jnp.zeros((NG, S), BF16)
    total = []
    for g in range(G):
        probs = p_ref[aligned(g * CH + local), :]
        tot = None
        for u in range(0, NG, 2):
            ps = [jnp.where(rows16 == jnp.asarray(u + w, BF16), probs, zero) for w in range(2)]
            vs = [vbuf[at + u + w, g] for w in range(2)]
            part = dot(jnp.concatenate(ps, axis=1), jnp.concatenate(vs, axis=0))
            tot = part if tot is None else tot + part
        total.append(tot)
    return total


def local_kernel(x_h, ga_h, ba_h, gm_h, bm_h, wq_h, wo_h, wu_h, wd_h, k_h, v_h, pos_s, pos_h,
                 ko_h, vo_h, q_o, kn_o, vn_o, m_o, part_o, x_v, wo_v, kp_o,
                 ln_v, wq_v, w32_v, wqb_v, wu_v, wd_v, kb, vb, pos_v, ain_v, min_v, cos_v, sin_v, h_v, qt_v, p_v, pn_v, ctx_v, a_v,
                 sem_in, sem_k, sem_v, sem_ko, sem_vo, sem_kp):
    ngr = R0 // NG

    def rd(src, dst, i):
        c = pltpu.make_async_copy(src, dst, sem_in.at[i])
        c.start()
        return c

    c_pos = rd(pos_h, pos_v, 0)
    c_x = [rd(x_h.at[pl.ds(64 * i, 64)], x_v.at[pl.ds(64 * i, 64)], 15 + i) for i in range(4)]
    c_ln = [rd(r, ln_v.at[pl.ds(8 * i, 1)], 2 + i) for i, r in enumerate((ga_h, ba_h, gm_h, bm_h))]
    c_wq = [rd(wq_h.at[pl.ds(3072 * i, 3072)], wq_v.at[pl.ds(3072 * i, 3072)], 6 + i) for i in range(4)]

    def kcopy(i, a, b, sem):
        return pltpu.make_async_copy(a.at[pl.ds(NG * i, NG)], b.at[pl.ds(NG * i, NG)], sem.at[i])

    kp_copies = [pltpu.make_async_copy(k_h.at[pl.ds(R0 + NG * i, NG)], kp_o.at[pl.ds(NG * i, NG)], sem_kp.at[i]) for i in range(PER)]

    c_pos.wait()
    lane = iota((S, H), 1)
    inv = jnp.exp((lane & (H // 2 - 1)).astype(F32) * (-2.0 * math.log(ROPE_BASE) / H))
    for i in range(2):
        at = jnp.broadcast_to(pos_v[pl.ds(i, 1), :].astype(F32), (S, H)).T
        ang = at * inv
        sn = jnp.sin(ang)
        cos_v[pl.ds(S * i, S), :] = jnp.cos(ang)
        sin_v[pl.ds(S * i, S), :] = jnp.where(lane < H // 2, -sn, sn)

    for c in c_ln + c_x:
        c.wait()
    for i in range(PER):
        kcopy(i, k_h, kb, sem_k).start()
    RB = 16
    NB = 4

    @pl.loop(0, B // (RB * NB))
    def _(i):
        rows = [pl.ds(pl.multiple_of(i * (RB * NB) + RB * w, RB), RB) for w in range(NB)]

        def tile(r, j):
            return x_v[r, pl.ds(128 * j, 128)].astype(F32)

        means, scales = [], []
        for r in rows:
            tot = tile(r, 0)
            for j in range(1, 16):
                tot = tot + tile(r, j)
            means.append(jnp.sum(tot, axis=-1, keepdims=True) * (1.0 / D))
        for r, mean in zip(rows, means):
            tot = jnp.zeros((RB, 128), F32)
            for j in range(16):
                d = tile(r, j) - mean
                tot = tot + d * d
            scales.append(lax.rsqrt(jnp.sum(tot, axis=-1, keepdims=True) * (1.0 / D) + LN_EPS))
        for r, mean, rs in zip(rows, means, scales):
            for j in range(16):
                cs = pl.ds(128 * j, 128)
                n = (tile(r, j) - mean) * rs
                ain_v[r, cs] = (n * ln_v[pl.ds(0, 1), cs] + ln_v[pl.ds(8, 1), cs]).astype(BF16)
                min_v[r, cs] = (n * ln_v[pl.ds(16, 1), cs] + ln_v[pl.ds(24, 1), cs]).astype(BF16)

    for c in c_wq:
        c.wait()
    for i in range(PER):
        kcopy(i, v_h, vb, sem_v).start()
    c_wo = rd(wo_h, wo_v, 10)
    c_wu = [rd(wu_h.at[pl.ds(1024 * i, 1024)], wu_v.at[pl.ds(1024 * i, 1024)], 11 + i) for i in range(2)]

    @pl.loop(0, 16)
    def _(i):
        w32_v[...] = wq_v[pl.ds(pl.multiple_of(i * 768, 768), 768), :].astype(F32)
        for j in range(3):
            for g in range(G):
                wqb_v[pl.ds(pl.multiple_of(i * 128, 128), 128), pl.ds((g * 3 + j) * H, H)] = (
                    w32_v[pl.ds(2 * j + g, 128, stride=6), :].astype(BF16))

    def rotary(u, r):
        return u * cos_v[r, :] + pltpu.roll(u, H // 2, 1) * sin_v[r, :]

    for n in range(3):
        qkv = dot(ain_v[...], wqb_v[:, pl.ds(256 * n, 256)]).astype(BF16).astype(F32)
        for w in range(2):
            g, j = divmod(2 * n + w, 3)
            u = qkv[:, w * H:(w + 1) * H]
            dst = (q_o, kn_o, vn_o)[j]
            if j < 2:
                u = rotary(u, pl.ds(0, B)).astype(BF16).astype(F32)
            dst[:, pl.ds(g * H, H)] = u

    for c in range(R0 // CH):
        c_wd = [rd(wd_h.at[pl.ds(512 * i, 512)], wd_v.at[pl.ds(512 * i, 512)], 13 + i) for i in range(2)]
        base = c * CH

        def wait_k(i, c=c):
            kcopy(c * PER + i, k_h, kb, sem_k).wait()

        def wait_v(i, c=c):
            kcopy(c * PER + i, v_h, vb, sem_v).wait()

        def old_v(i, c=c):
            if c > 0:
                add_rows(vb, vn_o, pos_s, base - CH + i * NG, base - CH + i * NG)

        def add_k(i):
            add_rows(kb, kn_o, pos_s, base + i * NG, base + i * NG)

        attend_scores(c, base, wait_k, old_v, kb, q_o, kn_o, pos_v, qt_v, p_v, pn_v)
        if c > 0:
            for j in range(PER):
                kcopy((c - 1) * PER + j, vb, vo_h, sem_vo).start()
        for cp in kp_copies:
            cp.start()
        attend_context(c, base, 0, PER, wait_v, add_k, vb, vn_o, p_v, pn_v, ctx_v)
        if c == 0:
            c_wo.wait()
        for n in range(8):
            a_v[pl.ds(base, CH), pl.ds(256 * n, 256)] = dot(ctx_v[...], wo_v[:, pl.ds(256 * n, 256)])
        for j in range(PER):
            kcopy(c * PER + j, kb, ko_h, sem_ko).start()

    for c in c_wu:
        c.wait()
    for n in range(4):
        u = dot(min_v[...], wu_v[:, pl.ds(256 * n, 256)])
        h_v[:, pl.ds(256 * n, 256)] = (0.5 * u * (1.0 + lax.erf(u * (2.0 ** -0.5)))).astype(BF16)
        for i in ((0, 1), (2,), (3,), ())[n]:
            add_rows(vb, vn_o, pos_s, R0 - CH + i * NG, R0 - CH + i * NG)
    for j in range(PER):
        kcopy(R0 // NG - PER + j, vb, vo_h, sem_vo).start()
    for c in c_wd:
        c.wait()
    for n in range(8):
        cs = pl.ds(256 * n, 256)
        m_o[:, cs] = dot(h_v[...], wd_v[:, cs])
        part_o[:, cs] = (a_v[:, cs] + m_o[pl.ds(0, R0), cs]).astype(BF16)

    for cp in kp_copies:
        cp.wait()
    for i in range(ngr):
        kcopy(i, kb, ko_h, sem_ko).wait()
        kcopy(i, vb, vo_h, sem_vo).wait()


PARTS = ((0, 64), (64, 64), (128, 64), (192, 32), (224, 32))


def reduce_kernel(k_h, v_h, q_i, kn_i, vn_i, m_i, part_i, x_v, wo_v, kp_i, pos_i,
                  k2, v2, out_o,
                  qt_v, p_v, pn_v, ctx_v, part_v, d2_v, sum_v, rs_v,
                  sem_k, sem_v, s_d, r_d, s_rs, r_rs, s_ag, r_ag, s_e, r_e):
    tp = lax.axis_index("tp")
    core = tp % 2
    chip = tp // 2
    first = R0 // CH
    per = CH // NG
    QC = D // 4

    def kcopy(i):
        return pltpu.make_async_copy(k_h.at[pl.ds(R0 + CH + NG * i, NG)], k2.at[pl.ds(NG * i, NG)], sem_k.at[i])

    def vcopy(i):
        return pltpu.make_async_copy(v_h.at[pl.ds(R0 + NG * i, NG)], v2.at[pl.ds(NG * i, NG)], sem_v.at[i])

    def issue_k(c):
        for i in range(per):
            kcopy((c - first - 1) * per + i).start()

    def issue_v(c):
        for i in range(per):
            vcopy((c - first) * per + i).start()

    issue_v(1)

    sib = tp + 1 - 2 * core
    peers = []
    for k in (3, 2, 1):
        chip_k = (chip // 2 + k // 2) % 2 * 2 + (chip % 2 + k % 2) % 2
        peers.append((chip_k, chip_k * 2 + core))

    barrier = pltpu.get_barrier_semaphore()
    for t in [sib] + [p for _, p in peers]:
        pl.semaphore_signal(barrier, inc=1, device_id={"tp": t}, device_id_type=MESH)
    my_cols = pl.ds(pl.multiple_of(chip * QC, QC), QC)

    def remote(src, dst, s, r, t):
        return pltpu.make_async_remote_copy(src_ref=src, dst_ref=dst, send_sem=s, recv_sem=r, device_id={"tp": t}, device_id_type=MESH)

    def part_of(c, which):
        start, n = PARTS[c]
        ref, base = (part_i, start) if start < R0 else (part_v, start - R0)
        return ref.at[pl.ds(pl.multiple_of(base + which * (n // 2), NG), n // 2)]

    def half(c):
        start, n = PARTS[c]
        return pl.ds(start // 2, n // 2)

    def out_rows(c):
        start, n = PARTS[c]
        return pl.ds(pl.multiple_of(start + core * (n // 2), NG), n // 2)

    def a_copy(c):
        return remote(part_of(c, 1 - core), d2_v.at[half(c)], s_d.at[c], r_d.at[c], sib)

    def b_copies(c):
        return [remote(sum_v.at[half(c), pl.ds(pl.multiple_of(ck * QC, QC), QC)], rs_v.at[k, half(c)], s_rs.at[c, k], r_rs.at[c, k], t)
                for k, (ck, t) in enumerate(peers)]

    def c_copies(c):
        piece = out_o.at[out_rows(c), my_cols]
        return [remote(piece, piece, s_ag.at[c, k], r_ag.at[c, k], t) for k, (_, t) in enumerate(peers)]

    def d_copy(c):
        rows = out_o.at[out_rows(c)]
        return remote(rows, rows, s_e.at[c], r_e.at[c], sib)

    def step_a(c):
        a_copy(c).start()

    def step_b(c):
        a_copy(c).wait_recv()
        sum_v[half(c)] = (part_of(c, core)[...].astype(F32) + d2_v[half(c)].astype(F32)).astype(BF16)
        for cp in b_copies(c):
            cp.start()

    def step_c(c):
        tot = sum_v[half(c), my_cols].astype(F32) + x_v[out_rows(c), my_cols].astype(F32)
        for k, cp in enumerate(b_copies(c)):
            cp.wait_recv()
            tot = tot + rs_v[k, half(c)].astype(F32)
        out_o[out_rows(c), my_cols] = tot.astype(BF16)
        for cp in c_copies(c):
            cp.start()

    def step_d(c):
        for cp in c_copies(c):
            cp.wait_recv()
        d_copy(c).start()

    def nothing(i):
        pass

    def scores(c, between):
        if c == first:
            attend_scores(c, 0, nothing, nothing, kp_i, q_i, kn_i, pos_i, qt_v, p_v, pn_v, between)
        else:
            at = (c - first - 1) * per
            attend_scores(c, at * NG, lambda i: kcopy(at + i).wait(), nothing, k2, q_i, kn_i, pos_i, qt_v, p_v, pn_v, between)

    def context(c, lo, hi, between):
        at = (c - first) * CH
        attend_context(c, at, lo, hi, lambda i: vcopy((c - first) * per + i).wait(), nothing, v2, vn_i, p_v, pn_v, ctx_v, between)
        n = (hi - lo) * NG
        for k in range(8):
            cs = pl.ds(256 * k, 256)
            part_v[pl.ds(at + lo * NG, n), cs] = (
                dot(ctx_v[pl.ds(lo * NG, n), :], wo_v[:, cs]) + m_i[pl.ds(c * CH + lo * NG, n), cs]).astype(BF16)

    pl.semaphore_wait(barrier, 4)
    step_a(0)
    def between1():
        issue_k(2)

    scores(1, between1)
    step_b(0)
    def between2():
        issue_v(2)

    context(1, 0, per, between2)
    step_a(1)
    def between3():
        issue_k(3)

    scores(2, between3)
    step_b(1)
    def between4():
        issue_v(3)

    context(2, 0, per, between4)
    step_a(2)
    def between5():
        step_b(2)

    scores(3, between5)
    step_c(0)
    def between6():
        pass

    context(3, 0, per // 2, between6)
    step_a(3)
    def between7():
        pass

    context(3, per // 2, per, between7)
    step_a(4)
    step_b(3)
    step_b(4)
    step_c(1)
    step_c(2)
    step_c(3)
    step_c(4)
    step_d(0)
    step_d(1)
    step_d(2)
    step_d(3)
    step_d(4)
    for c in range(len(PARTS)):
        a_copy(c).wait_send()
        for cp in b_copies(c):
            cp.wait_send()
        for cp in c_copies(c):
            cp.wait_send()
        d_copy(c).wait()


def write_kernel(kp_i, k_i, v_i, o_i, kn_i, vn_i, pos_s, k0_h, v0_h, kp3, k3, v3, ko_h, vo_h, o_h, sem):
    n = (B - R0) // NG
    c_out = pltpu.make_async_copy(o_i, o_h, sem.at[2 * n])
    c_out.start()

    def copy(src, dst, i, k):
        return pltpu.make_async_copy(src.at[pl.ds(NG * i, NG)], dst.at[pl.ds(R0 + NG * k, NG)], sem.at[k if dst is ko_h else n + k])

    late = None
    for src, dst, new, first, count in ((kp3, ko_h, kn_i, 0, PER), (v3, vo_h, vn_i, 0, n), (k3, ko_h, kn_i, PER, n - PER)):
        add_rows(src, new, pos_s, R0 + first * NG, 0)
        if late is not None:
            late.start()

        @pl.loop(1, count)
        def _(i, src=src, dst=dst, new=new, first=first):
            add_rows(src, new, pos_s, R0 + (first + i) * NG, i * NG)
            copy(src, dst, i - 1, first + i - 1).start()

        late = copy(src, dst, count - 1, first + count - 1)
    late.start()

    for src, dst, first, count in ((kp3, ko_h, 0, PER), (v3, vo_h, 0, n), (k3, ko_h, PER, n - PER)):
        @pl.loop(0, count)
        def _(i, src=src, dst=dst, first=first):
            copy(src, dst, i, first + i).wait()

    c_out.wait()


def solution(mesh):
    row_spec = P('dp', None)
    vec_spec = P(None)
    cache_spec = P('dp', 'tp', None, None)
    vm = pl.BlockSpec(memory_space=pltpu.VMEM)
    sm = pl.BlockSpec(memory_space=pltpu.SMEM)
    anyspace = pl.BlockSpec(memory_space=pl.ANY)
    dma = pltpu.SemaphoreType.DMA
    MIB = 1024 * 1024

    def hbm(t):
        return pltpu.with_memory_space_constraint(t, pltpu.HBM)

    def device_step(x, ln_attn_gamma, ln_attn_beta, ln_mlp_gamma, ln_mlp_beta, w_qkv, w_out, w_up, w_down, k_cache, v_cache, positions):
        wq = w_qkv.transpose(0, 2, 1, 3).reshape(D * 3 * G, H)
        wo = w_out.reshape(G * H, D)
        pos2 = positions.reshape(2, 128)
        cache = jax.ShapeDtypeStruct((B, G, S, H), BF16)
        NR = B - R0
        k0, v0, q, kn, vn, m, part, xv, wov, kp = pl.pallas_call(
            local_kernel,
            out_shape=(cache, cache) + (pltpu.VMEM((B, G * H), F32),) * 3 + (pltpu.VMEM((B, D), F32), pltpu.VMEM((R0, D), BF16), pltpu.VMEM((B, D), BF16),
                                                                              pltpu.VMEM((G * H, D), BF16), pltpu.VMEM((CH, G, S, H), BF16)),
            in_specs=[anyspace] * 11 + [sm, anyspace],
            out_specs=(anyspace, anyspace) + (vm,) * 8,
            scratch_shapes=[
                pltpu.VMEM((32, D), F32), pltpu.VMEM((D * 3 * G, H), BF16), pltpu.VMEM((768, H), F32),
                pltpu.VMEM((D, 768), BF16), pltpu.VMEM((D, FL), BF16), pltpu.VMEM((FL, D), BF16),
                pltpu.VMEM((R0, G, S, H), BF16), pltpu.VMEM((R0, G, S, H), BF16), pltpu.VMEM((2, 128), jnp.int32),
                pltpu.VMEM((B, D), BF16), pltpu.VMEM((B, D), BF16), pltpu.VMEM((B, H), F32), pltpu.VMEM((B, H), F32),
                pltpu.VMEM((B, FL), BF16), pltpu.VMEM((G * H, 2 * CH), BF16), pltpu.VMEM((2 * CH, S), BF16), pltpu.VMEM((2 * CH, H), F32),
                pltpu.VMEM((CH, G * H), BF16), pltpu.VMEM((R0, D), F32),
                dma((19,)), dma((R0 // NG,)), dma((R0 // NG,)), dma((R0 // NG,)), dma((R0 // NG,)), dma((PER,)),
            ],
            compiler_params=pltpu.CompilerParams(vmem_limit_bytes=38 * MIB),
            name="local_part",
        )(hbm(x), *[hbm(t.reshape(1, D)) for t in (ln_attn_gamma, ln_attn_beta, ln_mlp_gamma, ln_mlp_beta)],
          hbm(wq), hbm(wo), hbm(w_up), hbm(w_down), hbm(k_cache), hbm(v_cache), positions, hbm(pos2))

        n = len(PARTS)
        block = pltpu.VMEM((NR, G, S, H), BF16)
        kblock = pltpu.VMEM((NR - CH, G, S, H), BF16)
        kpblock = pltpu.VMEM((CH, G, S, H), BF16)
        k2, v2, o = pl.pallas_call(
            reduce_kernel,
            out_shape=(kblock, block, pltpu.VMEM((B, D), BF16)),
            in_specs=[anyspace] * 2 + [vm] * 9,
            out_specs=(vm,) * 3,
            scratch_shapes=[
                pltpu.VMEM((G * H, 2 * CH), BF16), pltpu.VMEM((2 * CH, S), BF16),
                pltpu.VMEM((2 * CH, H), F32), pltpu.VMEM((CH, G * H), BF16), pltpu.VMEM((NR, D), BF16), pltpu.VMEM((B // 2, D), BF16),
                pltpu.VMEM((B // 2, D), BF16), pltpu.VMEM((3, B // 2, D // 4), BF16),
                dma((NR // NG - PER,)), dma((NR // NG,)),
                dma((n,)), dma((n,)), dma((n, 3)), dma((n, 3)), dma((n, 3)), dma((n, 3)), dma((n,)), dma((n,)),
            ],
            compiler_params=pltpu.CompilerParams(vmem_limit_bytes=16 * MIB, collective_id=0, has_side_effects=True),
            name="reduce_part",
        )(hbm(k_cache), hbm(v_cache), q, kn, vn, m, part, xv, wov, kp, pos2)

        _, _, _, kf, vf, out = pl.pallas_call(
            write_kernel,
            out_shape=(kpblock, kblock, block, cache, cache, jax.ShapeDtypeStruct((B, D), BF16)),
            in_specs=[vm] * 6 + [sm] + [anyspace] * 2,
            out_specs=(vm,) * 3 + (anyspace,) * 3,
            scratch_shapes=[dma((2 * (NR // NG) + 1,))],
            input_output_aliases={0: 0, 1: 1, 2: 2, 7: 3, 8: 4},
            compiler_params=pltpu.CompilerParams(vmem_limit_bytes=4 * MIB),
            name="write_part",
        )(kp, k2, v2, o, kn, vn, positions, k0, v0)
        return out, kf, vf

    return jax.shard_map(device_step, mesh=mesh, in_specs=(row_spec, vec_spec, vec_spec, vec_spec, vec_spec, P(None, 'tp', None, None), P('tp', None, None, None), P(None, 'tp'), P('tp', None), cache_spec, cache_spec, P('dp')), out_specs=(row_spec, cache_spec, cache_spec), check_vma=False)
```

```python
import functools
import math

import jax
import jax.numpy as jnp
from jax import lax
from jax.experimental import pallas as pl
from jax.experimental.pallas import tpu as pltpu
from jax.sharding import PartitionSpec as P

LN_EPS = 1e-5
ROPE_BASE = 10000.0
NEG_BIG = -1e30
MESH = pl.DeviceIdType.MESH
F32 = jnp.float32
BF16 = jnp.bfloat16

B = 256
D = 2048
S = 128
H = 128
G = 2
FL = 1024
R0 = 64
CH = 64
NG = 16
GI = 2
SCALE = H ** -0.5
PER = CH // NG


def dot(a, b):
    return jnp.dot(a, b, preferred_element_type=F32)


def iota(shape, dim):
    return lax.broadcasted_iota(jnp.int32, shape, dim)


def build_queries(q_ref, row, qt_ref):
    stacked = jnp.concatenate([q_ref[pl.ds(row, CH), pl.ds(0, H)], q_ref[pl.ds(row, CH), pl.ds(H, H)]], axis=0)
    turned = stacked.T
    low = iota((H, 2 * CH), 1) < CH
    qt_ref[pl.ds(0, H), :] = jnp.where(low, turned, 0.0).astype(BF16)
    qt_ref[pl.ds(H, H), :] = jnp.where(low, 0.0, turned).astype(BF16)


def aligned(row):
    return pl.ds(row if isinstance(row, int) else pl.multiple_of(row, NG), NG)


def add_rows(buf, new_ref, pos_s, row, at):
    rows = aligned(row)
    new = [new_ref[rows, pl.ds(g * H, H)] for g in range(G)]
    inside = iota((NG, H), 0).astype(F32).astype(BF16)
    for u in range(NG):
        pos = pos_s[row + u]
        start = pl.multiple_of(lax.shift_left(lax.shift_right_logical(pos, 4), 4), NG)
        mask = inside == jnp.full((NG, H), (pos - start).astype(F32), F32).astype(BF16)
        for g in range(G):
            tile = buf.at[at + u, g, pl.ds(start, NG), :]
            tile[...] = jnp.where(mask, jnp.broadcast_to(new[g][u:u + 1], (NG, H)).astype(BF16), tile[...])


def scores_of_group(kbuf, qt_ref, acc, at, local):
    lane = iota((S, 2 * CH), 1) & (CH - 1)
    for u in range(NG):
        keys = jnp.concatenate([kbuf[at + u, g] for g in range(G)], axis=1)
        acc = jnp.where(lane == local + u, dot(keys, qt_ref[...]), acc)
    return acc


def attend_scores(c, at, wait, also, kbuf, q_ref, kn_ref, pos_v, qt_v, p_v, pn_v, between=None):
    build_queries(q_ref, c * CH, qt_v)
    rows = pl.ds(c * CH, CH)
    with_new = jnp.concatenate([q_ref[rows, pl.ds(g * H, H)] * kn_ref[rows, pl.ds(g * H, H)] for g in range(G)], axis=0)
    s_new = jnp.sum(with_new.T, axis=0, keepdims=True)
    new_at = pos_columns(pos_v, c)

    def step(j, acc):
        for w in range(GI):
            wait(j * GI + w)
        for w in range(GI):
            i = j * GI + w
            acc = scores_of_group(kbuf, qt_v, acc, at + i * NG, i * NG)
            also(i)
        return acc

    acc = jnp.zeros((S, 2 * CH), F32)
    if between is None:
        acc = lax.fori_loop(0, PER // GI, step, acc)
    else:
        for j in range(PER // GI):
            acc = step(j, acc)
            if j == 0:
                between()
    slot = iota((S, 2 * CH), 0)
    s = jnp.where(slot < new_at, acc * SCALE, jnp.where(slot == new_at, s_new * SCALE, NEG_BIG))
    p = softmax_slots(s).astype(BF16).astype(F32)
    p_v[...] = jnp.where(slot == new_at, 0.0, p).T.astype(BF16)
    p_new = jnp.sum(jnp.where(slot == new_at, p, 0.0), axis=0, keepdims=True)
    pn_v[...] = jnp.broadcast_to(p_new, (2 * CH, H)).T


def attend_context(c, at, lo, hi, wait, also, vbuf, vn_ref, p_v, pn_v, ctx_v, between=None):
    def step(j):
        for w in range(GI):
            wait(lo + j * GI + w)
        for w in range(GI):
            i = lo + j * GI + w
            ctx = context_of_group(vbuf, p_v, at + i * NG, i * NG)
            rows = aligned(c * CH + i * NG)
            for g in range(G):
                new = pn_v[aligned(g * CH + i * NG), :] * vn_ref[rows, pl.ds(g * H, H)]
                ctx_v[aligned(i * NG), pl.ds(g * H, H)] = (ctx[g] + new).astype(BF16)
            also(i)

    if between is None:
        pl.loop(0, (hi - lo) // GI)(step)
    else:
        for j in range((hi - lo) // GI):
            step(j)
            if j == 0:
                between()


def pos_columns(pos_v, chunk):
    row = pos_v[pl.ds(chunk // 2, 1), :]
    lane = iota((1, 2 * CH), 1)
    turned = pltpu.roll(row, CH, 1)
    return jnp.where(lane < CH, row, turned) if chunk % 2 == 0 else jnp.where(lane < CH, turned, row)


def softmax_slots(s):
    e = jnp.exp(s - jnp.max(s, axis=0, keepdims=True))
    return e / jnp.sum(e, axis=0, keepdims=True)


def context_of_group(vbuf, p_ref, at, local):
    rows16 = iota((NG, S), 0).astype(F32).astype(BF16)
    zero = jnp.zeros((NG, S), BF16)
    total = []
    for g in range(G):
        probs = p_ref[aligned(g * CH + local), :]
        tot = None
        for u in range(0, NG, 2):
            ps = [jnp.where(rows16 == jnp.asarray(u + w, BF16), probs, zero) for w in range(2)]
            vs = [vbuf[at + u + w, g] for w in range(2)]
            part = dot(jnp.concatenate(ps, axis=1), jnp.concatenate(vs, axis=0))
            tot = part if tot is None else tot + part
        total.append(tot)
    return total


def local_kernel(x_h, ga_h, ba_h, gm_h, bm_h, wq_h, wo_h, wu_h, wd_h, k_h, v_h, pos_s, pos_h,
                 ko_h, vo_h, q_o, kn_o, vn_o, m_o, part_o, x_v, wo_v, kp_o,
                 ln_v, wq_v, w32_v, wqb_v, wu_v, wd_v, kb, vb, pos_v, ain_v, min_v, cos_v, sin_v, h_v, qt_v, p_v, pn_v, ctx_v, a_v,
                 sem_in, sem_k, sem_v, sem_ko, sem_vo, sem_kp):
    ngr = R0 // NG

    def rd(src, dst, i):
        c = pltpu.make_async_copy(src, dst, sem_in.at[i])
        c.start()
        return c

    c_pos = rd(pos_h, pos_v, 0)
    c_x = [rd(x_h.at[pl.ds(64 * i, 64)], x_v.at[pl.ds(64 * i, 64)], 15 + i) for i in range(4)]
    c_ln = [rd(r, ln_v.at[pl.ds(8 * i, 1)], 2 + i) for i, r in enumerate((ga_h, ba_h, gm_h, bm_h))]
    c_wq = [rd(wq_h.at[pl.ds(3072 * i, 3072)], wq_v.at[pl.ds(3072 * i, 3072)], 6 + i) for i in range(4)]

    def kcopy(i, a, b, sem):
        return pltpu.make_async_copy(a.at[pl.ds(NG * i, NG)], b.at[pl.ds(NG * i, NG)], sem.at[i])

    kp_copies = [pltpu.make_async_copy(k_h.at[pl.ds(R0 + NG * i, NG)], kp_o.at[pl.ds(NG * i, NG)], sem_kp.at[i]) for i in range(PER)]

    c_pos.wait()
    lane = iota((S, H), 1)
    inv = jnp.exp((lane & (H // 2 - 1)).astype(F32) * (-2.0 * math.log(ROPE_BASE) / H))
    for i in range(2):
        at = jnp.broadcast_to(pos_v[pl.ds(i, 1), :].astype(F32), (S, H)).T
        ang = at * inv
        sn = jnp.sin(ang)
        cos_v[pl.ds(S * i, S), :] = jnp.cos(ang)
        sin_v[pl.ds(S * i, S), :] = jnp.where(lane < H // 2, -sn, sn)

    for c in c_ln + c_x:
        c.wait()
    for i in range(PER):
        kcopy(i, k_h, kb, sem_k).start()
    RB = 16
    NB = 4

    @pl.loop(0, B // (RB * NB))
    def _(i):
        rows = [pl.ds(pl.multiple_of(i * (RB * NB) + RB * w, RB), RB) for w in range(NB)]

        def tile(r, j):
            return x_v[r, pl.ds(128 * j, 128)].astype(F32)

        means, scales = [], []
        for r in rows:
            tot = tile(r, 0)
            for j in range(1, 16):
                tot = tot + tile(r, j)
            means.append(jnp.sum(tot, axis=-1, keepdims=True) * (1.0 / D))
        for r, mean in zip(rows, means):
            tot = jnp.zeros((RB, 128), F32)
            for j in range(16):
                d = tile(r, j) - mean
                tot = tot + d * d
            scales.append(lax.rsqrt(jnp.sum(tot, axis=-1, keepdims=True) * (1.0 / D) + LN_EPS))
        for r, mean, rs in zip(rows, means, scales):
            for j in range(16):
                cs = pl.ds(128 * j, 128)
                n = (tile(r, j) - mean) * rs
                ain_v[r, cs] = (n * ln_v[pl.ds(0, 1), cs] + ln_v[pl.ds(8, 1), cs]).astype(BF16)
                min_v[r, cs] = (n * ln_v[pl.ds(16, 1), cs] + ln_v[pl.ds(24, 1), cs]).astype(BF16)

    for c in c_wq:
        c.wait()
    for i in range(PER):
        kcopy(i, v_h, vb, sem_v).start()
    c_wo = rd(wo_h, wo_v, 10)
    c_wu = [rd(wu_h.at[pl.ds(1024 * i, 1024)], wu_v.at[pl.ds(1024 * i, 1024)], 11 + i) for i in range(2)]

    @pl.loop(0, 16)
    def _(i):
        w32_v[...] = wq_v[pl.ds(pl.multiple_of(i * 768, 768), 768), :].astype(F32)
        for j in range(3):
            for g in range(G):
                wqb_v[pl.ds(pl.multiple_of(i * 128, 128), 128), pl.ds((g * 3 + j) * H, H)] = (
                    w32_v[pl.ds(2 * j + g, 128, stride=6), :].astype(BF16))

    def rotary(u, r):
        return u * cos_v[r, :] + pltpu.roll(u, H // 2, 1) * sin_v[r, :]

    for n in range(3):
        qkv = dot(ain_v[...], wqb_v[:, pl.ds(256 * n, 256)]).astype(BF16).astype(F32)
        for w in range(2):
            g, j = divmod(2 * n + w, 3)
            u = qkv[:, w * H:(w + 1) * H]
            dst = (q_o, kn_o, vn_o)[j]
            if j < 2:
                u = rotary(u, pl.ds(0, B)).astype(BF16).astype(F32)
            dst[:, pl.ds(g * H, H)] = u

    for c in range(R0 // CH):
        c_wd = [rd(wd_h.at[pl.ds(512 * i, 512)], wd_v.at[pl.ds(512 * i, 512)], 13 + i) for i in range(2)]
        base = c * CH

        def wait_k(i, c=c):
            kcopy(c * PER + i, k_h, kb, sem_k).wait()

        def wait_v(i, c=c):
            kcopy(c * PER + i, v_h, vb, sem_v).wait()

        def old_v(i, c=c):
            if c > 0:
                add_rows(vb, vn_o, pos_s, base - CH + i * NG, base - CH + i * NG)

        def add_k(i):
            add_rows(kb, kn_o, pos_s, base + i * NG, base + i * NG)

        attend_scores(c, base, wait_k, old_v, kb, q_o, kn_o, pos_v, qt_v, p_v, pn_v)
        if c > 0:
            for j in range(PER):
                kcopy((c - 1) * PER + j, vb, vo_h, sem_vo).start()
        for cp in kp_copies:
            cp.start()
        attend_context(c, base, 0, PER, wait_v, add_k, vb, vn_o, p_v, pn_v, ctx_v)
        if c == 0:
            c_wo.wait()
        for n in range(8):
            a_v[pl.ds(base, CH), pl.ds(256 * n, 256)] = dot(ctx_v[...], wo_v[:, pl.ds(256 * n, 256)])
        for j in range(PER):
            kcopy(c * PER + j, kb, ko_h, sem_ko).start()

    for c in c_wu:
        c.wait()
    for n in range(4):
        u = dot(min_v[...], wu_v[:, pl.ds(256 * n, 256)])
        h_v[:, pl.ds(256 * n, 256)] = (0.5 * u * (1.0 + lax.erf(u * (2.0 ** -0.5)))).astype(BF16)
        for i in ((0, 1), (2,), (3,), ())[n]:
            add_rows(vb, vn_o, pos_s, R0 - CH + i * NG, R0 - CH + i * NG)
    for j in range(PER):
        kcopy(R0 // NG - PER + j, vb, vo_h, sem_vo).start()
    for c in c_wd:
        c.wait()
    for n in range(8):
        cs = pl.ds(256 * n, 256)
        m_o[:, cs] = dot(h_v[...], wd_v[:, cs])
        part_o[:, cs] = (a_v[:, cs] + m_o[pl.ds(0, R0), cs]).astype(BF16)

    for cp in kp_copies:
        cp.wait()
    for i in range(ngr):
        kcopy(i, kb, ko_h, sem_ko).wait()
        kcopy(i, vb, vo_h, sem_vo).wait()


PARTS = ((0, 64), (64, 64), (128, 64), (192, 32), (224, 32))


def reduce_kernel(k_h, v_h, q_i, kn_i, vn_i, m_i, part_i, x_v, wo_v, kp_i, pos_i,
                  k2, v2, out_o,
                  qt_v, p_v, pn_v, ctx_v, part_v, d2_v, sum_v, rs_v,
                  sem_k, sem_v, s_d, r_d, s_rs, r_rs, s_ag, r_ag, s_e, r_e):
    tp = lax.axis_index("tp")
    core = tp % 2
    chip = tp // 2
    first = R0 // CH
    per = CH // NG
    QC = D // 4

    def kcopy(i):
        return pltpu.make_async_copy(k_h.at[pl.ds(R0 + CH + NG * i, NG)], k2.at[pl.ds(NG * i, NG)], sem_k.at[i])

    def vcopy(i):
        return pltpu.make_async_copy(v_h.at[pl.ds(R0 + NG * i, NG)], v2.at[pl.ds(NG * i, NG)], sem_v.at[i])

    def issue_k(c):
        for i in range(per):
            kcopy((c - first - 1) * per + i).start()

    def issue_v(c):
        for i in range(per):
            vcopy((c - first) * per + i).start()

    issue_v(1)

    sib = tp + 1 - 2 * core
    peers = []
    for k in (3, 2, 1):
        chip_k = (chip // 2 + k // 2) % 2 * 2 + (chip % 2 + k % 2) % 2
        peers.append((chip_k, chip_k * 2 + core))

    barrier = pltpu.get_barrier_semaphore()
    for t in [sib] + [p for _, p in peers]:
        pl.semaphore_signal(barrier, inc=1, device_id={"tp": t}, device_id_type=MESH)
    my_cols = pl.ds(pl.multiple_of(chip * QC, QC), QC)

    def remote(src, dst, s, r, t):
        return pltpu.make_async_remote_copy(src_ref=src, dst_ref=dst, send_sem=s, recv_sem=r, device_id={"tp": t}, device_id_type=MESH)

    def part_of(c, which):
        start, n = PARTS[c]
        ref, base = (part_i, start) if start < R0 else (part_v, start - R0)
        return ref.at[pl.ds(pl.multiple_of(base + which * (n // 2), NG), n // 2)]

    def half(c):
        start, n = PARTS[c]
        return pl.ds(start // 2, n // 2)

    def out_rows(c):
        start, n = PARTS[c]
        return pl.ds(pl.multiple_of(start + core * (n // 2), NG), n // 2)

    def a_copy(c):
        return remote(part_of(c, 1 - core), d2_v.at[half(c)], s_d.at[c], r_d.at[c], sib)

    def b_copies(c):
        return [remote(sum_v.at[half(c), pl.ds(pl.multiple_of(ck * QC, QC), QC)], rs_v.at[k, half(c)], s_rs.at[c, k], r_rs.at[c, k], t)
                for k, (ck, t) in enumerate(peers)]

    def c_copies(c):
        piece = out_o.at[out_rows(c), my_cols]
        return [remote(piece, piece, s_ag.at[c, k], r_ag.at[c, k], t) for k, (_, t) in enumerate(peers)]

    def d_copy(c):
        rows = out_o.at[out_rows(c)]
        return remote(rows, rows, s_e.at[c], r_e.at[c], sib)

    def step_a(c):
        a_copy(c).start()

    def step_b(c):
        a_copy(c).wait_recv()
        sum_v[half(c)] = (part_of(c, core)[...].astype(F32) + d2_v[half(c)].astype(F32)).astype(BF16)
        for cp in b_copies(c):
            cp.start()

    def step_c(c):
        tot = sum_v[half(c), my_cols].astype(F32) + x_v[out_rows(c), my_cols].astype(F32)
        for k, cp in enumerate(b_copies(c)):
            cp.wait_recv()
            tot = tot + rs_v[k, half(c)].astype(F32)
        out_o[out_rows(c), my_cols] = tot.astype(BF16)
        for cp in c_copies(c):
            cp.start()

    def step_d(c):
        for cp in c_copies(c):
            cp.wait_recv()
        d_copy(c).start()

    def nothing(i):
        pass

    def scores(c, between):
        if c == first:
            attend_scores(c, 0, nothing, nothing, kp_i, q_i, kn_i, pos_i, qt_v, p_v, pn_v, between)
        else:
            at = (c - first - 1) * per
            attend_scores(c, at * NG, lambda i: kcopy(at + i).wait(), nothing, k2, q_i, kn_i, pos_i, qt_v, p_v, pn_v, between)

    def context(c, lo, hi, between):
        at = (c - first) * CH
        attend_context(c, at, lo, hi, lambda i: vcopy((c - first) * per + i).wait(), nothing, v2, vn_i, p_v, pn_v, ctx_v, between)
        n = (hi - lo) * NG
        for k in range(8):
            cs = pl.ds(256 * k, 256)
            part_v[pl.ds(at + lo * NG, n), cs] = (
                dot(ctx_v[pl.ds(lo * NG, n), :], wo_v[:, cs]) + m_i[pl.ds(c * CH + lo * NG, n), cs]).astype(BF16)

    pl.semaphore_wait(barrier, 4)
    step_a(0)
    def between1():
        issue_k(2)

    scores(1, between1)
    step_b(0)
    def between2():
        issue_v(2)

    context(1, 0, per, between2)
    step_a(1)
    def between3():
        issue_k(3)

    scores(2, between3)
    step_b(1)
    def between4():
        issue_v(3)

    context(2, 0, per, between4)
    step_a(2)
    step_c(0)
    def between5():
        step_b(2)

    scores(3, between5)
    def between6():
        pass

    context(3, 0, per // 2, between6)
    step_a(3)
    def between7():
        pass

    context(3, per // 2, per, between7)
    step_a(4)
    step_b(3)
    step_b(4)
    step_c(1)
    step_c(2)
    step_c(3)
    step_c(4)
    step_d(0)
    step_d(1)
    step_d(2)
    step_d(3)
    step_d(4)
    for c in range(len(PARTS)):
        a_copy(c).wait_send()
        for cp in b_copies(c):
            cp.wait_send()
        for cp in c_copies(c):
            cp.wait_send()
        d_copy(c).wait()


def write_kernel(kp_i, k_i, v_i, o_i, kn_i, vn_i, pos_s, k0_h, v0_h, kp3, k3, v3, ko_h, vo_h, o_h, sem):
    n = (B - R0) // NG
    c_out = pltpu.make_async_copy(o_i, o_h, sem.at[2 * n])
    c_out.start()

    def copy(src, dst, i, k):
        return pltpu.make_async_copy(src.at[pl.ds(NG * i, NG)], dst.at[pl.ds(R0 + NG * k, NG)], sem.at[k if dst is ko_h else n + k])

    late = None
    for src, dst, new, first, count in ((kp3, ko_h, kn_i, 0, PER), (v3, vo_h, vn_i, 0, n), (k3, ko_h, kn_i, PER, n - PER)):
        add_rows(src, new, pos_s, R0 + first * NG, 0)
        if late is not None:
            late.start()

        @pl.loop(1, count)
        def _(i, src=src, dst=dst, new=new, first=first):
            add_rows(src, new, pos_s, R0 + (first + i) * NG, i * NG)
            copy(src, dst, i - 1, first + i - 1).start()

        late = copy(src, dst, count - 1, first + count - 1)
    late.start()

    for src, dst, first, count in ((kp3, ko_h, 0, PER), (v3, vo_h, 0, n), (k3, ko_h, PER, n - PER)):
        @pl.loop(0, count)
        def _(i, src=src, dst=dst, first=first):
            copy(src, dst, i, first + i).wait()

    c_out.wait()


def solution(mesh):
    row_spec = P('dp', None)
    vec_spec = P(None)
    cache_spec = P('dp', 'tp', None, None)
    vm = pl.BlockSpec(memory_space=pltpu.VMEM)
    sm = pl.BlockSpec(memory_space=pltpu.SMEM)
    anyspace = pl.BlockSpec(memory_space=pl.ANY)
    dma = pltpu.SemaphoreType.DMA
    MIB = 1024 * 1024

    def hbm(t):
        return pltpu.with_memory_space_constraint(t, pltpu.HBM)

    def device_step(x, ln_attn_gamma, ln_attn_beta, ln_mlp_gamma, ln_mlp_beta, w_qkv, w_out, w_up, w_down, k_cache, v_cache, positions):
        wq = w_qkv.transpose(0, 2, 1, 3).reshape(D * 3 * G, H)
        wo = w_out.reshape(G * H, D)
        pos2 = positions.reshape(2, 128)
        cache = jax.ShapeDtypeStruct((B, G, S, H), BF16)
        NR = B - R0
        k0, v0, q, kn, vn, m, part, xv, wov, kp = pl.pallas_call(
            local_kernel,
            out_shape=(cache, cache) + (pltpu.VMEM((B, G * H), F32),) * 3 + (pltpu.VMEM((B, D), F32), pltpu.VMEM((R0, D), BF16), pltpu.VMEM((B, D), BF16),
                                                                              pltpu.VMEM((G * H, D), BF16), pltpu.VMEM((CH, G, S, H), BF16)),
            in_specs=[anyspace] * 11 + [sm, anyspace],
            out_specs=(anyspace, anyspace) + (vm,) * 8,
            scratch_shapes=[
                pltpu.VMEM((32, D), F32), pltpu.VMEM((D * 3 * G, H), BF16), pltpu.VMEM((768, H), F32),
                pltpu.VMEM((D, 768), BF16), pltpu.VMEM((D, FL), BF16), pltpu.VMEM((FL, D), BF16),
                pltpu.VMEM((R0, G, S, H), BF16), pltpu.VMEM((R0, G, S, H), BF16), pltpu.VMEM((2, 128), jnp.int32),
                pltpu.VMEM((B, D), BF16), pltpu.VMEM((B, D), BF16), pltpu.VMEM((B, H), F32), pltpu.VMEM((B, H), F32),
                pltpu.VMEM((B, FL), BF16), pltpu.VMEM((G * H, 2 * CH), BF16), pltpu.VMEM((2 * CH, S), BF16), pltpu.VMEM((2 * CH, H), F32),
                pltpu.VMEM((CH, G * H), BF16), pltpu.VMEM((R0, D), F32),
                dma((19,)), dma((R0 // NG,)), dma((R0 // NG,)), dma((R0 // NG,)), dma((R0 // NG,)), dma((PER,)),
            ],
            compiler_params=pltpu.CompilerParams(vmem_limit_bytes=38 * MIB),
            name="local_part",
        )(hbm(x), *[hbm(t.reshape(1, D)) for t in (ln_attn_gamma, ln_attn_beta, ln_mlp_gamma, ln_mlp_beta)],
          hbm(wq), hbm(wo), hbm(w_up), hbm(w_down), hbm(k_cache), hbm(v_cache), positions, hbm(pos2))

        n = len(PARTS)
        block = pltpu.VMEM((NR, G, S, H), BF16)
        kblock = pltpu.VMEM((NR - CH, G, S, H), BF16)
        kpblock = pltpu.VMEM((CH, G, S, H), BF16)
        k2, v2, o = pl.pallas_call(
            reduce_kernel,
            out_shape=(kblock, block, pltpu.VMEM((B, D), BF16)),
            in_specs=[anyspace] * 2 + [vm] * 9,
            out_specs=(vm,) * 3,
            scratch_shapes=[
                pltpu.VMEM((G * H, 2 * CH), BF16), pltpu.VMEM((2 * CH, S), BF16),
                pltpu.VMEM((2 * CH, H), F32), pltpu.VMEM((CH, G * H), BF16), pltpu.VMEM((NR, D), BF16), pltpu.VMEM((B // 2, D), BF16),
                pltpu.VMEM((B // 2, D), BF16), pltpu.VMEM((3, B // 2, D // 4), BF16),
                dma((NR // NG - PER,)), dma((NR // NG,)),
                dma((n,)), dma((n,)), dma((n, 3)), dma((n, 3)), dma((n, 3)), dma((n, 3)), dma((n,)), dma((n,)),
            ],
            compiler_params=pltpu.CompilerParams(vmem_limit_bytes=16 * MIB, collective_id=0, has_side_effects=True),
            name="reduce_part",
        )(hbm(k_cache), hbm(v_cache), q, kn, vn, m, part, xv, wov, kp, pos2)

        _, _, _, kf, vf, out = pl.pallas_call(
            write_kernel,
            out_shape=(kpblock, kblock, block, cache, cache, jax.ShapeDtypeStruct((B, D), BF16)),
            in_specs=[vm] * 6 + [sm] + [anyspace] * 2,
            out_specs=(vm,) * 3 + (anyspace,) * 3,
            scratch_shapes=[dma((2 * (NR // NG) + 1,))],
            input_output_aliases={0: 0, 1: 1, 2: 2, 7: 3, 8: 4},
            compiler_params=pltpu.CompilerParams(vmem_limit_bytes=4 * MIB),
            name="write_part",
        )(kp, k2, v2, o, kn, vn, positions, k0, v0)
        return out, kf, vf

    return jax.shard_map(device_step, mesh=mesh, in_specs=(row_spec, vec_spec, vec_spec, vec_spec, vec_spec, P(None, 'tp', None, None), P('tp', None, None, None), P(None, 'tp'), P('tp', None), cache_spec, cache_spec, P('dp')), out_specs=(row_spec, cache_spec, cache_spec), check_vma=False)
```
